32 devices in a mesh: rep: 8 (over z, x), shard: 4 (over y, core).
Axes of the slice: x: 2, y: 2, z: 4, core: 2. Of those that a mesh axis runs over, the one named last changes fastest.
Arguments:
- frames: bfloat16 [32, 1024, 512], P(('rep', 'shard')), may hold values from -6 to 6
- segments: int32 [32, 1024], P(('rep', 'shard')), may hold values from 0 to 1, as said below
- padding: int32 [32, 1024], P(('rep', 'shard')), may hold values from 0 to 1, as said below
- masked: int32 [32, 384], P(('rep', 'shard')), may hold values from 0 to 1023, as said below
- distract: int32 [32, 384, 100], P(('rep', 'shard')), may hold values from 0 to 1023, as said below
- targets: int32 [32, 1024], P(('rep', 'shard')), may hold values from 0 to 639
- params: float32 [12566528], P('shard'), may hold values from -4 to 4
- first_moment: float32 [12566528], P('shard'), may hold values from -0.375 to 0.375
- second_moment: float32 [12566528], P('shard'), may hold values from 0.00013750815 to 0.0022001304
Outputs:
- weight_step: float32 [12566528], P('shard')
- first_moment_new: float32 [12566528], P('shard')
- second_moment_new: float32 [12566528], P('shard')
- grad_norm: float32 [], replicated
- loss_total: float32 [], replicated
The draws below stay inside these ranges and needn't reach their ends.
Inputs may be any that keep to these rules, and one draw needn't show every extreme that they name: `segments`: each row holds two whole clips one after the other, numbered 0 and 1, one of them of 750 frames; the empty slots at the row's end carry number 1. `padding`: padding is a run of one or more slots at the end of each row. `masked`: 384 distinct frames of the row, none of them padding, in rising order. `distract`: frames of the same clip as the masked frame, never that frame itself, drawn with replacement.
All inputs are finite; a program needn't handle non-finite values.
Results may differ from the reference program's by a relative error of at most 0.012.
The reference program's roundings to bfloat16 on the way count: a program that leaves them out, or rounds other values in their place, can miss the bound.
Values may be sent and summed in bfloat16 or wider, within the bound.
A program may use at most 576 MiB of HBM per device.

```python
import math
import jax
import jax.numpy as jnp
from jax import lax

D = 768
HEADS = 12
HEAD_DIM = 64
FF = 3072
FEAT = 512
TAPS = 128
GROUPS = 16
FINAL = 256
CODES = 640
NEG = 100
LONG = 750
ROW = 1024
MASK_ROW = 384
NROWS = 32
NPAR = 12566528


def clip_plan(key):
    short_len = jax.random.randint(jax.random.fold_in(key, 11), (NROWS,), (ROW - LONG) // 2, ROW - LONG)
    long_first = jax.random.randint(jax.random.fold_in(key, 12), (NROWS,), 0, 2)
    first_len = jnp.where(long_first == 1, LONG, short_len).astype(jnp.int32)
    used_len = (LONG + short_len).astype(jnp.int32)
    positions = jnp.arange(ROW, dtype=jnp.int32)[None, :]
    segment = (positions >= first_len[:, None]).astype(jnp.int32)
    pad_flag = (positions >= used_len[:, None]).astype(jnp.int32)
    return (first_len, used_len, segment, pad_flag)


def masked_plan(key):
    first_len, used_len, segment, pad_flag = clip_plan(key)
    row_keys = jax.random.split(jax.random.fold_in(key, 13), NROWS)
    orders = jax.vmap(lambda row_key: jax.random.permutation(row_key, ROW))(row_keys).astype(jnp.int32)
    priority = orders + ROW * pad_flag
    chosen = jnp.argsort(priority, axis=1)[:, :MASK_ROW]
    return jnp.sort(chosen, axis=1).astype(jnp.int32)


def draw_segments(key, part):
    return clip_plan(key)[2]


def draw_padding(key, part):
    return clip_plan(key)[3]


def draw_masked(key, part):
    return masked_plan(key)


def draw_distract(key, part):
    first_len, used_len, segment, pad_flag = clip_plan(key)
    chosen = masked_plan(key)
    in_second = jnp.take_along_axis(segment, chosen, 1)
    clip_start = in_second * first_len[:, None]
    clip_len = jnp.where(in_second == 1, used_len[:, None] - first_len[:, None], first_len[:, None])
    offset_in = chosen - clip_start
    raw_pick = jax.random.randint(jax.random.fold_in(key, 14), (NROWS, MASK_ROW, NEG), 0, clip_len[:, :, None] - 1)
    skipped = raw_pick + (raw_pick >= offset_in[:, :, None]).astype(jnp.int32)
    return (clip_start[:, :, None] + skipped).astype(jnp.int32)


def set_ends(array, own_key, smallest, largest):
    dims = array.shape
    place = [jax.random.randint(jax.random.fold_in(own_key, axis), (), 0, dims[axis]) for axis in range(len(dims))]
    array = array.at[tuple(place)].set(smallest)
    longest = dims.index(max(dims))
    place[longest] = (place[longest] + 1) % dims[longest]
    return array.at[tuple(place)].set(largest)


def shard_levels(stream_key, dims, cuts, least, top_value):
    level = 1.0
    for axis_at, parts in cuts:
        heights = jax.random.uniform(jax.random.fold_in(jax.random.fold_in(stream_key, 6), axis_at), (parts,), jnp.float32, least / len(cuts), top_value / len(cuts))
        level = level * jnp.repeat(jnp.exp(heights), dims[axis_at] // parts).reshape((-1,) + (1,) * (len(dims) - 1 - axis_at))
    return level


def centred(key, dims, scale, bound, cuts=(), kind=jnp.bfloat16):
    loudness = shard_levels(key, dims, cuts, -0.22, 0.18) if cuts else 1.0
    array = jax.random.normal(key, dims, jnp.float32) * scale * loudness
    return jnp.minimum(jnp.maximum(array, -bound), bound).astype(kind)


def setup_inputs(seed: int = 0) -> dict:
    splits = jax.random.split(jax.random.key(seed), 10)
    frames = centred(splits[0], (NROWS, ROW, FEAT), 1.0, 6.0, ((0, 32),))
    segments = draw_segments(jax.random.fold_in(splits[9], 71), 0)
    padding = draw_padding(jax.random.fold_in(splits[9], 71), 0)
    masked = draw_masked(jax.random.fold_in(splits[9], 71), 0)
    distract = draw_distract(jax.random.fold_in(splits[9], 71), 0)
    targets = set_ends(jax.random.randint(splits[5], (NROWS, ROW), 0, CODES), jax.random.fold_in(splits[5], 1), 0, CODES - 1).astype(jnp.int32)
    params = centred(splits[6], (NPAR,), 1.0, 4.0, ((0, 4),), jnp.float32)
    first_moment = centred(splits[7], (NPAR,), (12 * (NROWS * MASK_ROW) ** 0.5 * FINAL ** -0.5 * NPAR ** -0.5), 0.375, ((0, 4),), jnp.float32)
    second_moment = jnp.clip(jnp.exp(math.log(0.0022001304) - 2.7725887 * jax.random.uniform(splits[8], (NPAR,), jnp.float32) ** shard_levels(splits[8], (NPAR,), ((0, 4),), -0.2, 0.2)), 0.00013750815, 0.0022001304)
    return dict(frames=frames, segments=segments, padding=padding, masked=masked, distract=distract, targets=targets, params=params, first_moment=first_moment, second_moment=second_moment)


highest = lax.Precision.HIGHEST
inverse_temp = 10.0

@jax.custom_vjp
def low(v):
    return lax.optimization_barrier(v.astype(jnp.bfloat16)).astype(jnp.float32)

@jax.custom_vjp
def low_back(v):
    return v

def low_keep(v):
    return (low(v), None)

def low_pass(kept, grad):
    return (grad,)

def back_keep(v):
    return (v, None)

def back_low(kept, grad):
    return (low(grad),)
low.defvjp(low_keep, low_pass)
low_back.defvjp(back_keep, back_low)

def layout():
    group_width = D // GROUPS
    return [('feat_gain', (FEAT,)), ('feat_bias', (FEAT,)), ('proj_in', (FEAT, D)), ('proj_bias', (D,)), ('mask_vector', (D,)), ('pos_weight', (TAPS, GROUPS, group_width, group_width)), ('pos_bias', (D,)), ('enc_gain', (D,)), ('enc_bias', (D,)), ('qkv_weight', (D, 3 * D)), ('query_bias', (D,)), ('value_bias', (D,)), ('out_weight', (D, D)), ('out_bias', (D,)), ('attn_gain', (D,)), ('attn_bias', (D,)), ('up_weight', (D, FF)), ('up_bias', (FF,)), ('down_weight', (FF, D)), ('down_bias', (D,)), ('ffn_gain', (D,)), ('ffn_bias', (D,)), ('final_weight', (D, FINAL)), ('final_bias', (FINAL,)), ('codebook', (CODES, FINAL))]

def unpack(flat):
    result = {}
    offset = 0
    for key_name, dims_shape in layout():
        entry_count = math.prod(dims_shape)
        result[key_name] = flat[offset:offset + entry_count].reshape(dims_shape)
        offset = offset + entry_count
    return result

def layer_norm(values, gain_raw, bias_raw):
    centered = values - lax.optimization_barrier(jnp.mean(values, -1, keepdims=True))
    scale_inv = lax.rsqrt(lax.optimization_barrier(jnp.mean(centered * centered, -1, keepdims=True)) + 1e-05)
    return centered * scale_inv * (1.0 + 0.2 * gain_raw) + 0.2 * bias_raw

def gelu_exact(values):
    return jax.nn.gelu(values, approximate=False)

def contrast(context, codebook, masked_row, distract_row, target_row):
    picked = jnp.take(context, masked_row, axis=0)
    picked_unit = picked * lax.rsqrt(lax.optimization_barrier(jnp.sum(picked * picked, -1, keepdims=True)) + 1e-06)
    code_unit = codebook * lax.rsqrt(lax.optimization_barrier(jnp.sum(codebook * codebook, -1, keepdims=True)) + 1e-06)
    similar = jnp.dot(picked_unit, code_unit.T, precision=highest, preferred_element_type=jnp.float32)
    candidate = jnp.concatenate([masked_row[:, None], distract_row], 1)
    code_rows = jnp.take(target_row, candidate)
    logits = jnp.take_along_axis(similar, code_rows, 1) * inverse_temp
    column = lax.broadcasted_iota(jnp.int32, code_rows.shape, 1)
    dropped = (code_rows == code_rows[:, :1]) & (column > 0)
    logits = jnp.where(dropped, -1e+30, logits)
    return jnp.sum(jax.nn.logsumexp(logits, axis=1) - logits[:, 0])

def adam_update(weight_old, grad_scaled, first_old, second_old):
    first_new = 0.5 * first_old + 0.5 * grad_scaled
    second_new = 0.5 * second_old + 0.5 * grad_scaled * grad_scaled
    first_hat = first_new / (1.0 - 0.5 ** 4)
    second_hat = second_new / (1.0 - 0.5 ** 4)
    weight_delta = -0.1 * (first_hat / (jnp.sqrt(second_hat) + 1e-08) + 0.01 * weight_old)
    return (weight_delta, first_new, second_new)

def conv_reference(source, pos_weight, segment):
    half_taps = TAPS // 2
    group_width = D // GROUPS
    padded = jnp.pad(source, ((half_taps, half_taps), (0, 0)))
    seg_pad = jnp.pad(segment, (half_taps, half_taps), constant_values=-1)

    def one_tap(accum, inputs):
        tap_index, tap_weight = inputs
        shifted = lax.dynamic_slice_in_dim(padded, tap_index, ROW, 0)
        shifted_seg = lax.dynamic_slice_in_dim(seg_pad, tap_index, ROW, 0)
        keep_tap = (shifted_seg == segment).astype(jnp.float32)
        shifted = (shifted * keep_tap[:, None]).reshape(ROW, GROUPS, group_width)
        return (accum + jnp.einsum('tgc,gco->tgo', shifted, tap_weight, precision=highest), None)
    start_acc = jnp.zeros((ROW, GROUPS, group_width), jnp.float32)
    result, _ = lax.scan(one_tap, start_acc, (jnp.arange(TAPS, dtype=jnp.int32), pos_weight))
    return result.reshape(ROW, D)

def row_loss(weights, frames_row, segment, padding_row, masked_row, distract_row, target_row):
    keep_frame = (1 - padding_row).astype(jnp.float32)
    hidden_in = low(layer_norm(frames_row, weights['feat_gain'], weights['feat_bias']))
    projected = low_back(jnp.dot(hidden_in, weights['proj_in'], precision=highest) * FEAT ** (-0.5) + 0.2 * weights['proj_bias'])
    flagged = jnp.zeros((ROW,), jnp.float32).at[masked_row].set(1.0)
    replaced = jnp.where(flagged[:, None] > 0, weights['mask_vector'][None, :], projected)
    conv_in = low(replaced * keep_frame[:, None])
    conv_out = low_back(conv_reference(conv_in, weights['pos_weight'], segment) * (TAPS * D // GROUPS) ** (-0.5) + 0.2 * weights['pos_bias'])
    embedded = replaced + gelu_exact(conv_out)
    normed = layer_norm(embedded, weights['enc_gain'], weights['enc_bias'])
    qkv_bias = jnp.concatenate([0.2 * weights['query_bias'], jnp.zeros((D,), jnp.float32), 0.2 * weights['value_bias']])
    qkv_all = low(low_back(jnp.dot(low(normed), weights['qkv_weight'], precision=highest) * D ** (-0.5) + qkv_bias))
    queries = qkv_all[:, :D].reshape(ROW, HEADS, HEAD_DIM)
    keys_all = qkv_all[:, D:2 * D].reshape(ROW, HEADS, HEAD_DIM)
    values_all = qkv_all[:, 2 * D:].reshape(ROW, HEADS, HEAD_DIM)
    allowed = (segment[:, None] == segment[None, :]) & (padding_row[None, :] == 0)
    scores = low_back(jnp.einsum('qhd,khd->hqk', queries, keys_all, precision=highest) * HEAD_DIM ** (-0.5))
    scores = jnp.where(allowed[None], scores, -1e+30)
    probs = low(jax.nn.softmax(scores, axis=-1))
    mixed = low(low_back(jnp.einsum('hqk,khd->qhd', probs, values_all, precision=highest).reshape(ROW, D)))
    attended = low_back(jnp.dot(mixed, weights['out_weight'], precision=highest) * (LONG / D) ** 0.5 + 0.2 * weights['out_bias'])
    first = layer_norm(normed + attended, weights['attn_gain'], weights['attn_bias'])
    hidden_ff = low_back(jnp.dot(low(first), weights['up_weight'], precision=highest) * D ** (-0.5) + 0.2 * weights['up_bias'])
    activated = low(gelu_exact(hidden_ff))
    branch = low_back(jnp.dot(activated, weights['down_weight'], precision=highest) * FF ** (-0.5) + 0.2 * weights['down_bias'])
    second = layer_norm(first + branch, weights['ffn_gain'], weights['ffn_bias'])
    context = low_back(jnp.dot(low(second), weights['final_weight'], precision=highest) * D ** (-0.5) + 0.2 * weights['final_bias'])
    return contrast(context, weights['codebook'], masked_row, distract_row, target_row)

def reference(frames, segments, padding, masked, distract, targets, params, first_moment, second_moment):

    def total_loss(flat):
        weights = unpack(low(flat))

        def one_row(accum, row_data):
            return (accum + jax.checkpoint(row_loss)(weights, *row_data), None)
        summed, _ = lax.scan(one_row, jnp.float32(0.0), (frames.astype(jnp.float32), segments, padding, masked, distract, targets))
        return summed
    loss_sum, pullback = jax.vjp(total_loss, params)
    gradient = pullback(jnp.ones_like(loss_sum))[0]
    grad_norm = jnp.sqrt(jnp.sum(gradient * gradient))
    clip_limit = 12.0 * math.sqrt(MASK_ROW * NROWS / FINAL)
    factor = jnp.minimum(1.0, clip_limit / (grad_norm + 1e-06))
    weight_delta, first_new, second_new = adam_update(params, gradient * factor, first_moment, second_moment)
    return (weight_delta, first_new, second_new, grad_norm, loss_sum)
```

```python
import functools
import math

import jax
import jax.numpy as jnp
from jax import lax
from jax.experimental import pallas as pl
from jax.experimental.pallas import tpu as pltpu
from jax.sharding import PartitionSpec as P

D = 768
HEADS = 12
HEAD_DIM = 64
FF = 3072
FEAT = 512
TAPS = 128
GROUPS = 16
FINAL = 256
CODES = 640
LONG = 750
ROW = 1024


LANE = 128
WIDTH = D // GROUPS
HALF = D // 2
HALF_GROUPS = 8
GAP = TAPS // 2
TQ = ROW + GAP + 16
VMEM_MAX = 66_000_000
highest = lax.Precision.HIGHEST
inverse_temp = 10.0


def layout():
    return [
        ("feat_gain", (FEAT,)),
        ("feat_bias", (FEAT,)),
        ("proj_in", (FEAT, D)),
        ("proj_bias", (D,)),
        ("mask_vector", (D,)),
        ("pos_weight", (TAPS, GROUPS, WIDTH, WIDTH)),
        ("pos_bias", (D,)),
        ("enc_gain", (D,)),
        ("enc_bias", (D,)),
        ("qkv_weight", (D, 3 * D)),
        ("query_bias", (D,)),
        ("value_bias", (D,)),
        ("out_weight", (D, D)),
        ("out_bias", (D,)),
        ("attn_gain", (D,)),
        ("attn_bias", (D,)),
        ("up_weight", (D, FF)),
        ("up_bias", (FF,)),
        ("down_weight", (FF, D)),
        ("down_bias", (D,)),
        ("ffn_gain", (D,)),
        ("ffn_bias", (D,)),
        ("final_weight", (D, FINAL)),
        ("final_bias", (FINAL,)),
        ("codebook", (CODES, FINAL)),
    ]


def offsets():
    result = {}
    offset = 0
    for key_name, dims in layout():
        result[key_name] = offset
        offset += math.prod(dims)
    return result, offset


def unpack(flat):
    starts, _ = offsets()
    result = {}
    for key_name, dims in layout():
        if key_name != "pos_weight":
            start = starts[key_name]
            result[key_name] = flat[start : start + math.prod(dims)].reshape(dims)
    return result


def layer_norm(values, gain_raw, bias_raw):
    centered = values - jnp.mean(values, -1, keepdims=True)
    scale_inv = lax.rsqrt(jnp.mean(centered * centered, -1, keepdims=True) + 1e-05)
    return centered * scale_inv * (1.0 + 0.2 * gain_raw) + 0.2 * bias_raw


def gelu_exact(values):
    return jax.nn.gelu(values, approximate=False)


def adam_update(weight_old, grad_scaled, first_old, second_old):
    first_new = 0.5 * first_old + 0.5 * grad_scaled
    second_new = 0.5 * second_old + 0.5 * grad_scaled * grad_scaled
    first_hat = first_new / (1.0 - 0.5**4)
    second_hat = second_new / (1.0 - 0.5**4)
    weight_delta = -0.1 * (first_hat / (jnp.sqrt(second_hat) + 1e-08) + 0.01 * weight_old)
    return (weight_delta, first_new, second_new)


def swap_plan(bit):
    plans = []
    for keep in (0, 1):
        tiles = []
        for v in range(3):
            found = {}
            for lane in range(LANE):
                at = v * LANE + lane
                high = 1 if (at // WIDTH) & bit else 0
                source = at + WIDTH * bit * (keep - high)
                key = (high, source // LANE, (lane - source) % LANE)
                runs = found.setdefault(key, [])
                if runs and runs[-1][1] == lane:
                    runs[-1][1] = lane + 1
                else:
                    runs.append([lane, lane + 1])
            tiles.append(sorted(found.items(), key=lambda e: -sum(h - l for l, h in e[1])))
        plans.append(tiles)
    return plans


PLANS = {bit: swap_plan(bit) for bit in (4, 2, 1)}


def lane_runs(shape, runs):
    lane = lax.broadcasted_iota(jnp.int32, shape, 1)
    result = None
    for low, high in runs:
        part = None
        if low > 0:
            part = lane >= low
        if high < LANE:
            part = lane < high if part is None else part & (lane < high)
        result = part if result is None else result | part
    return result


def swap_half(pair, bit, keep):
    turned = {}

    def source(key):
        array, tile, turn = key
        if key not in turned:
            value = pair[array][tile]
            turned[key] = pltpu.roll(value, turn, 1) if turn else value
        return turned[key]

    result = []
    for entries in PLANS[bit][keep]:
        value = source(entries[0][0])
        for key, runs in entries[1:]:
            value = jnp.where(lane_runs(value.shape, runs), source(key), value)
        result.append(value)
    return result


def swap_slots(arrays):
    arrays = list(arrays)
    for bit in (4, 2, 1):
        done = list(arrays)
        for i in range(8):
            if i & bit == 0:
                pair = (arrays[i], arrays[i | bit])
                done[i] = swap_half(pair, bit, 0)
                done[i | bit] = swap_half(pair, bit, 1)
        arrays = done
    return arrays


def fold_slots(near, far, near_next, far_next, bit):
    kept = swap_half((near, far), bit, 0)
    moved = swap_half((near_next, far_next), bit, 1)
    return [a + b for a, b in zip(kept, moved)]


def load3(ref, lead, rows):
    return [ref[lead + (k, rows)] for k in range(3)]


def store3(ref, lead, rows, value):
    for k in range(3):
        ref[lead + (k, rows)] = value[k]


def weight_pack_kernel(w_ref, o_ref, flat, packed, *, lead):
    flat[...] = w_ref[...].astype(jnp.float32)
    for gh in range(2):
        for cb in range(6):
            taps = []
            for l in range(8):
                base = lead + l * 288 + gh * 144 + 3 * cb
                taps.append([flat[pl.ds(base + k, 8, stride=18), :] for k in range(3)])
            outs = swap_slots(taps)
            for ci in range(8):
                store3(packed, (), pl.ds(gh * 384 + 8 * cb + ci, 8, stride=48), outs[ci])
    for k in range(3):
        o_ref[:, :, k * LANE : (k + 1) * LANE] = (
            packed[k].reshape(GROUPS, WIDTH, LANE).astype(jnp.bfloat16)
        )


def pack_weights(flat_rows, first_row):
    lead = first_row % 16
    start = first_row - lead
    return pl.pallas_call(
        functools.partial(weight_pack_kernel, lead=lead),
        grid=(16,),
        in_specs=[
            pl.BlockSpec((pl.Element(2304 + 16), pl.Element(LANE)), lambda i: (pl.multiple_of(start + 2304 * i, 16), 0))
        ],
        out_specs=pl.BlockSpec((GROUPS, WIDTH, HALF), lambda i: (0, i // 2, i % 2)),
        out_shape=jax.ShapeDtypeStruct((GROUPS, HALF, D), jnp.bfloat16),
        scratch_shapes=[
            pltpu.VMEM((2304 + 16, LANE), jnp.float32),
            pltpu.VMEM((3, GROUPS * WIDTH, LANE), jnp.float32),
        ],
        compiler_params=pltpu.CompilerParams(vmem_limit_bytes=VMEM_MAX),
        name="weight_pack",
    )(flat_rows)


def weight_unpack_kernel(w_ref, o_ref, flat, packed, *, scale):
    for k in range(3):
        packed[k] = (
            w_ref[:, :, k * LANE : (k + 1) * LANE].reshape(GROUPS * WIDTH, LANE) * scale
        )
    for gh in range(2):
        for cb in range(6):
            outs = swap_slots(
                [
                    load3(packed, (), pl.ds(gh * 384 + 8 * cb + ci, 8, stride=48))
                    for ci in range(8)
                ]
            )
            for l in range(8):
                base = l * 288 + gh * 144 + 3 * cb
                for k in range(3):
                    flat[pl.ds(base + k, 8, stride=18), :] = outs[l][k]
    o_ref[...] = flat[...].astype(o_ref.dtype)


def unpack_weights(packed, scale, dtype):
    return pl.pallas_call(
        functools.partial(weight_unpack_kernel, scale=scale),
        grid=(16,),
        in_specs=[pl.BlockSpec((GROUPS, WIDTH, HALF), lambda i: (0, i // 2, i % 2))],
        out_specs=pl.BlockSpec((2304, LANE), lambda i: (i, 0)),
        out_shape=jax.ShapeDtypeStruct((16 * 2304, LANE), dtype),
        scratch_shapes=[
            pltpu.VMEM((2304, LANE), jnp.float32),
            pltpu.VMEM((3, GROUPS * WIDTH, LANE), jnp.float32),
        ],
        compiler_params=pltpu.CompilerParams(vmem_limit_bytes=VMEM_MAX),
        name="weight_unpack",
    )(packed)


def rows_at(start, count):
    return pl.ds(start, count)


def conv_fwd_kernel(edge_ref, x_ref, w_ref, y_ref, xs_ref, xs_all, zs, v_all, c1, d1, e1):
    g = pl.program_id(1)

    @pl.when(g == 0)
    def _():
        def build(i, carry):
            t0 = pl.multiple_of(i * 16, 16)
            outs = swap_slots(
                [
                    [x_ref[pl.ds(t0 + 16 * a, 16), k * LANE : (k + 1) * LANE] for k in range(3)]
                    for a in range(8)
                ]
            )
            for q in range(8):
                for k in range(3):
                    xs_all[q, pl.ds(t0, 16), k * LANE : (k + 1) * LANE] = outs[q][k]
            return carry

        lax.fori_loop(0, TQ // 16, build, 0)

    xs_ref[0] = xs_all[g]
    for c in range(3):
        z = jnp.dot(
            xs_all[g, c * 368 : (c + 1) * 368, :],
            w_ref[0],
            preferred_element_type=jnp.float32,
        )
        for k in range(6):
            zs[k, c * 368 : (c + 1) * 368, :] = z[:, k * LANE : (k + 1) * LANE]

    def add_high(i, carry):
        t0 = pl.multiple_of(i * 48, 8)
        for k in range(3):
            v_all[g, k, pl.ds(t0, 48), :] = (
                zs[k, pl.ds(t0, 48), :] + zs[k + 3, pl.ds(t0 + 8, 48), :]
            )
        return carry

    lax.fori_loop(0, TQ // 48, add_high, 0)

    @pl.when(g == HALF_GROUPS - 1)
    def _():
        def fold(src, dst, count, bit):
            def body(i, carry):
                t0 = pl.multiple_of(i * 16, 16)
                for p in range(count):
                    value = fold_slots(
                        load3(src, (p,), pl.ds(t0, 16)),
                        load3(src, (p + count,), pl.ds(t0, 16)),
                        load3(src, (p,), pl.ds(t0 + bit, 16)),
                        load3(src, (p + count,), pl.ds(t0 + bit, 16)),
                        bit,
                    )
                    store3(dst, (p,), pl.ds(t0, 16), value)
                return carry

            return body

        lax.fori_loop(0, TQ // 16, fold(v_all, c1, 4, 4), 0)
        lax.fori_loop(0, TQ // 16, fold(c1, d1, 2, 2), 0)
        lax.fori_loop(0, TQ // 16, fold(d1, e1, 1, 1), 0)
        edge = edge_ref[0]

        def place(i, carry):
            t0 = pl.multiple_of(i * 16, 16)
            row = t0 + lax.broadcasted_iota(jnp.int32, (16, LANE), 0)
            for k in range(3):
                y_ref[pl.ds(t0, 16), k * LANE : (k + 1) * LANE] = jnp.where(
                    row < edge, e1[0, k, pl.ds(t0, 16), :], e1[0, k, pl.ds(t0 + GAP, 16), :]
                )
            return carry

        lax.fori_loop(0, ROW // 16, place, 0)


def conv_forward(edge, x_gap, packed):
    rows = TQ + 16
    return pl.pallas_call(
        conv_fwd_kernel,
        grid_spec=pltpu.PrefetchScalarGridSpec(
            num_scalar_prefetch=1,
            grid=(2, HALF_GROUPS),
            in_specs=[
                pl.BlockSpec((ROW + 3 * GAP, HALF), lambda h, g, e: (0, h)),
                pl.BlockSpec((1, HALF, D), lambda h, g, e: (h * HALF_GROUPS + g, 0, 0)),
            ],
            out_specs=[
                pl.BlockSpec((ROW, HALF), lambda h, g, e: (0, h)),
                pl.BlockSpec((1, TQ, HALF), lambda h, g, e: (h * HALF_GROUPS + g, 0, 0)),
            ],
            scratch_shapes=[
                pltpu.VMEM((HALF_GROUPS, TQ, HALF), jnp.bfloat16),
                pltpu.VMEM((6, rows, LANE), jnp.float32),
                pltpu.VMEM((8, 3, rows, LANE), jnp.float32),
                pltpu.VMEM((4, 3, rows, LANE), jnp.float32),
                pltpu.VMEM((2, 3, rows, LANE), jnp.float32),
                pltpu.VMEM((1, 3, rows, LANE), jnp.float32),
            ],
        ),
        out_shape=[
            jax.ShapeDtypeStruct((ROW, D), jnp.float32),
            jax.ShapeDtypeStruct((GROUPS, TQ, HALF), jnp.bfloat16),
        ],
        compiler_params=pltpu.CompilerParams(vmem_limit_bytes=VMEM_MAX),
        cost_estimate=pl.CostEstimate(flops=60_000_000_000, bytes_accessed=60_000_000, transcendentals=0),
        name="conv_fwd",
    )(edge, x_gap, packed)


BACK = ROW + 3 * GAP


def conv_bwd_kernel(
    edge_ref, dy_ref, xs_ref, w_ref, dx_ref, dw_ref, dys, dl, dz, dxs, d1, e1
):
    g = pl.program_id(1)

    @pl.when(g == 0)
    def _():
        def spread(i, carry):
            t0 = pl.multiple_of(i * 16, 16)
            part = dy_ref[pl.ds(t0, 16), :].astype(jnp.float32)
            store3(dys, (), pl.ds(t0, 16), [part[:, k * LANE : (k + 1) * LANE] for k in range(3)])
            return carry

        lax.fori_loop(0, 1136 // 16, spread, 0)

        def build(i, carry):
            u0 = pl.multiple_of(i * 16, 16)
            outs = swap_slots([load3(dys, (), pl.ds(u0 + 8 - l, 16)) for l in range(8)])
            for q in range(8):
                store3(dl, (q,), pl.ds(u0, 16), outs[q])
            return carry

        lax.fori_loop(0, 1120 // 16, build, 0)
        zero = jnp.zeros((16, LANE), jnp.float32)

        def clear(i, carry):
            for q in range(8):
                for k in range(3):
                    dxs[q, k, pl.ds(pl.multiple_of(i * 16, 16), 16), :] = zero
            return carry

        lax.fori_loop(0, GAP // 16, clear, 0)
        lax.fori_loop((GAP + TQ) // 16, BACK // 16, clear, 0)

    def pack(i, carry):
        t0 = pl.multiple_of(i * 16, 16)
        for k in range(3):
            dz[pl.ds(t0, 16), k * LANE : (k + 1) * LANE] = dl[g, k, pl.ds(t0 + 8, 16), :].astype(
                jnp.bfloat16
            )
            dz[pl.ds(t0, 16), HALF + k * LANE : HALF + (k + 1) * LANE] = dl[
                g, k, pl.ds(t0, 16), :
            ].astype(jnp.bfloat16)
        return carry

    lax.fori_loop(0, TQ // 16, pack, 0)
    dw_ref[0] = lax.dot_general(
        xs_ref[0], dz[...], (((0,), (0,)), ((), ())), preferred_element_type=jnp.float32
    )
    for c in range(3):
        back = lax.dot_general(
            dz[c * 368 : (c + 1) * 368, :],
            w_ref[0],
            (((1,), (1,)), ((), ())),
            preferred_element_type=jnp.float32,
        )
        for k in range(3):
            dxs[g, k, GAP + c * 368 : GAP + (c + 1) * 368, :] = back[:, k * LANE : (k + 1) * LANE]

    @pl.when(g == HALF_GROUPS - 1)
    def _():
        def fold(src, dst, count, bit, first):
            def body(i, carry):
                t0 = pl.multiple_of(i * 16, 16)
                for p in range(count):
                    value = fold_slots(
                        load3(src, (p,), pl.ds(t0, 16)),
                        load3(src, (p + count,), pl.ds(t0, 16)),
                        load3(src, (p,), pl.ds(t0 - 16 * bit, 16)),
                        load3(src, (p + count,), pl.ds(t0 - 16 * bit, 16)),
                        bit,
                    )
                    store3(dst, (p,), pl.ds(t0, 16), value)
                return carry

            lax.fori_loop(first // 16, BACK // 16, body, 0)

        fold(dxs, dl, 4, 4, 64)
        fold(dl, d1, 2, 2, 96)
        fold(d1, e1, 1, 1, 112)
        edge = edge_ref[0]

        def place(i, carry):
            t0 = pl.multiple_of(i * 16, 16)
            row = t0 + lax.broadcasted_iota(jnp.int32, (16, LANE), 0)
            for k in range(3):
                dx_ref[pl.ds(t0, 16), k * LANE : (k + 1) * LANE] = jnp.where(
                    row < edge,
                    e1[0, k, pl.ds(t0 + 2 * GAP, 16), :],
                    e1[0, k, pl.ds(t0 + 3 * GAP, 16), :],
                )
            return carry

        lax.fori_loop(0, ROW // 16, place, 0)


def conv_backward(edge, dy_gap, shifted, packed):
    return pl.pallas_call(
        conv_bwd_kernel,
        grid_spec=pltpu.PrefetchScalarGridSpec(
            num_scalar_prefetch=1,
            grid=(2, HALF_GROUPS),
            in_specs=[
                pl.BlockSpec((1136, HALF), lambda h, g, e: (0, h)),
                pl.BlockSpec((1, TQ, HALF), lambda h, g, e: (h * HALF_GROUPS + g, 0, 0)),
                pl.BlockSpec((1, HALF, D), lambda h, g, e: (h * HALF_GROUPS + g, 0, 0)),
            ],
            out_specs=[
                pl.BlockSpec((ROW, HALF), lambda h, g, e: (0, h)),
                pl.BlockSpec((1, HALF, D), lambda h, g, e: (h * HALF_GROUPS + g, 0, 0)),
            ],
            scratch_shapes=[
                pltpu.VMEM((3, 1136, LANE), jnp.float32),
                pltpu.VMEM((8, 3, BACK, LANE), jnp.float32),
                pltpu.VMEM((TQ, D), jnp.bfloat16),
                pltpu.VMEM((8, 3, BACK, LANE), jnp.float32),
                pltpu.VMEM((2, 3, BACK, LANE), jnp.float32),
                pltpu.VMEM((1, 3, BACK, LANE), jnp.float32),
            ],
        ),
        out_shape=[
            jax.ShapeDtypeStruct((ROW, D), jnp.float32),
            jax.ShapeDtypeStruct((GROUPS, HALF, D), jnp.float32),
        ],
        compiler_params=pltpu.CompilerParams(vmem_limit_bytes=VMEM_MAX),
        cost_estimate=pl.CostEstimate(flops=90_000_000_000, bytes_accessed=80_000_000, transcendentals=0),
        name="conv_bwd",
    )(edge, dy_gap, shifted, packed)


def with_gap(values, edge, before, total):
    near = jnp.pad(values, ((before, total - ROW - before), (0, 0)))
    far = jnp.pad(values, ((before + GAP, total - ROW - before - GAP), (0, 0)))
    row = lax.broadcasted_iota(jnp.int32, (total, 1), 0) - before
    zero = jnp.zeros((), values.dtype)
    return jnp.where(row < edge, near, jnp.where(row >= edge + GAP, far, zero))


def head_scores(q_ref, k_ref, segq_ref, segk_ref, sub, rows):
    cols = slice(sub * HEAD_DIM, (sub + 1) * HEAD_DIM)
    scores = lax.dot_general(
        q_ref[rows, cols], k_ref[:, cols], (((1,), (1,)), ((), ())),
        preferred_element_type=jnp.float32,
    ) * HEAD_DIM ** (-0.5)
    allowed = segq_ref[rows, :] == segk_ref[...]
    scores = jnp.where(allowed, scores, -1e30)
    power = jnp.exp(scores - jnp.max(scores, -1, keepdims=True))
    return power * (1.0 / jnp.sum(power, -1, keepdims=True))


def attn_fwd_kernel(q_ref, k_ref, v_ref, segq_ref, segk_ref, o_ref):
    for block in range(q_ref.shape[0] // LANE):
        rows = slice(block * LANE, (block + 1) * LANE)
        parts = []
        for sub in range(2):
            probs = head_scores(q_ref, k_ref, segq_ref, segk_ref, sub, rows)
            parts.append(
                jnp.dot(
                    probs.astype(jnp.bfloat16),
                    v_ref[:, sub * HEAD_DIM : (sub + 1) * HEAD_DIM],
                    preferred_element_type=jnp.float32,
                )
            )
        o_ref[rows, :] = jnp.concatenate(parts, 1).astype(jnp.bfloat16)


def attn_bwd_kernel(
    q_ref, k_ref, v_ref, g_ref, segq_ref, segk_ref, dq_ref, dk_ref, dv_ref, probs_low, ds_low
):
    for sub in range(2):
        cols = slice(sub * HEAD_DIM, (sub + 1) * HEAD_DIM)
        for block in range(q_ref.shape[0] // LANE):
            rows = slice(block * LANE, (block + 1) * LANE)
            probs = head_scores(q_ref, k_ref, segq_ref, segk_ref, sub, rows)
            probs_low[rows, :] = probs.astype(jnp.bfloat16)
            grad_probs = lax.dot_general(
                g_ref[rows, cols], v_ref[:, cols], (((1,), (1,)), ((), ())),
                preferred_element_type=jnp.float32,
            )
            total = jnp.sum(probs * grad_probs, -1, keepdims=True)
            ds_low[rows, :] = (probs * (grad_probs - total)).astype(jnp.bfloat16)
        scale = HEAD_DIM ** (-0.5)
        turn = (((0,), (0,)), ((), ()))
        dv_ref[:, cols] = lax.dot_general(
            probs_low[...], g_ref[:, cols], turn, preferred_element_type=jnp.float32
        ).astype(jnp.bfloat16)
        dk_ref[:, cols] = (
            lax.dot_general(
                ds_low[...], q_ref[:, cols], turn, preferred_element_type=jnp.float32
            )
            * scale
        ).astype(jnp.bfloat16)
        dq_ref[:, cols] = (
            jnp.dot(ds_low[...], k_ref[:, cols], preferred_element_type=jnp.float32) * scale
        ).astype(jnp.bfloat16)


def attention(queries, kv, segq, segk):
    count = queries.shape[0]
    pairs = HEADS // 2
    return pl.pallas_call(
        attn_fwd_kernel,
        grid=(pairs,),
        in_specs=[
            pl.BlockSpec((count, LANE), lambda h: (0, h)),
            pl.BlockSpec((ROW, LANE), lambda h: (0, h)),
            pl.BlockSpec((ROW, LANE), lambda h: (0, pairs + h)),
            pl.BlockSpec((count, 1), lambda h: (0, 0)),
            pl.BlockSpec((1, ROW), lambda h: (0, 0)),
        ],
        out_specs=pl.BlockSpec((count, LANE), lambda h: (0, h)),
        out_shape=jax.ShapeDtypeStruct((count, D), jnp.bfloat16),
        compiler_params=pltpu.CompilerParams(vmem_limit_bytes=VMEM_MAX // 2),
        name="attn_fwd",
    )(queries, kv, kv, segq, segk)


def attention_back(queries, kv, grad, segq, segk):
    count = queries.shape[0]
    pairs = HEADS // 2
    return pl.pallas_call(
        attn_bwd_kernel,
        grid=(pairs,),
        in_specs=[
            pl.BlockSpec((count, LANE), lambda h: (0, h)),
            pl.BlockSpec((ROW, LANE), lambda h: (0, h)),
            pl.BlockSpec((ROW, LANE), lambda h: (0, pairs + h)),
            pl.BlockSpec((count, LANE), lambda h: (0, h)),
            pl.BlockSpec((count, 1), lambda h: (0, 0)),
            pl.BlockSpec((1, ROW), lambda h: (0, 0)),
        ],
        out_specs=[
            pl.BlockSpec((count, LANE), lambda h: (0, h)),
            pl.BlockSpec((ROW, LANE), lambda h: (0, h)),
            pl.BlockSpec((ROW, LANE), lambda h: (0, h)),
        ],
        out_shape=[
            jax.ShapeDtypeStruct((count, D), jnp.bfloat16),
            jax.ShapeDtypeStruct((ROW, D), jnp.bfloat16),
            jax.ShapeDtypeStruct((ROW, D), jnp.bfloat16),
        ],
        scratch_shapes=[
            pltpu.VMEM((count, ROW), jnp.bfloat16),
            pltpu.VMEM((count, ROW), jnp.bfloat16),
        ],
        compiler_params=pltpu.CompilerParams(vmem_limit_bytes=VMEM_MAX // 2),
        name="attn_bwd",
    )(queries, kv, kv, grad, segq, segk)


def dot_low(left, right):
    return jnp.dot(left, right, preferred_element_type=jnp.float32)


def dot_turn(left, right):
    return lax.dot_general(
        left, right, (((0,), (0,)), ((), ())), preferred_element_type=jnp.float32
    )


def dot_back(left, right):
    return lax.dot_general(
        left, right, (((1,), (1,)), ((), ())), preferred_element_type=jnp.float32
    )


def contrast_counts(masked_row, distract_row, target_row):
    frame = lax.broadcasted_iota(jnp.int32, (1, 1, ROW), 2)
    seen = jnp.sum((distract_row[:, :, None] == frame).astype(jnp.float32), 1)
    code = lax.broadcasted_iota(jnp.int32, (ROW, CODES), 1)
    is_code = (target_row[:, None] == code).astype(jnp.bfloat16)
    counts = dot_low(seen.astype(jnp.bfloat16), is_code)
    pick = (masked_row[:, None] == lax.broadcasted_iota(jnp.int32, (1, ROW), 1)).astype(
        jnp.bfloat16
    )
    own = dot_low(pick, is_code)
    return pick, own, jnp.where(own > 0, 1.0, counts)


def contrast(picked, codebook, own, weight):
    picked_unit = picked * lax.rsqrt(jnp.sum(picked * picked, -1, keepdims=True) + 1e-06)
    code_unit = codebook * lax.rsqrt(jnp.sum(codebook * codebook, -1, keepdims=True) + 1e-06)
    logits = inverse_temp * jnp.dot(
        picked_unit, code_unit.T, precision=highest, preferred_element_type=jnp.float32
    )
    logits = jnp.where(weight > 0, logits, -1e30)
    top = lax.stop_gradient(jnp.max(logits, -1, keepdims=True))
    total = jnp.sum(weight * jnp.exp(logits - top), -1)
    return jnp.sum(top[:, 0] + jnp.log(total) - jnp.sum(own * logits, -1))


def column_sum(rounded):
    return 0.2 * jnp.sum(rounded.astype(jnp.float32), 0)


def row_step(
    weights,
    packed,
    frames_row,
    segment,
    padding_row,
    masked_row,
    distract_row,
    target_row,
    before_conv=None,
):
    def vector(key_name):
        return weights[key_name].astype(jnp.float32)

    pick, own, weight = contrast_counts(masked_row, distract_row, target_row)
    edge = jnp.sum((segment == 0).astype(jnp.int32)).reshape(1)
    keep_frame = (1 - padding_row).astype(jnp.float32)
    hidden_in, feat_back = jax.vjp(
        layer_norm, frames_row.astype(jnp.float32), vector("feat_gain"), vector("feat_bias")
    )
    hidden_low = hidden_in.astype(jnp.bfloat16)
    projected = dot_low(hidden_low, weights["proj_in"]) * FEAT ** (-0.5) + 0.2 * vector("proj_bias")
    flagged = jnp.any(
        masked_row[None, :] == lax.broadcasted_iota(jnp.int32, (ROW, 1), 0), 1, keepdims=True
    )
    replaced = jnp.where(flagged, vector("mask_vector")[None, :], projected)
    conv_in = (replaced * keep_frame[:, None]).astype(jnp.bfloat16)
    pos_scale = (TAPS * D // GROUPS) ** (-0.5)
    conv_sum, shifted = conv_forward(edge, with_gap(conv_in, edge[0], GAP, ROW + 3 * GAP), packed)
    conv_out = conv_sum * pos_scale + 0.2 * vector("pos_bias")
    activated_pos, gelu_pos_back = jax.vjp(gelu_exact, conv_out)
    normed, enc_back = jax.vjp(
        layer_norm, replaced + activated_pos, vector("enc_gain"), vector("enc_bias")
    )
    normed_low = normed.astype(jnp.bfloat16)
    pick32 = pick.astype(jnp.float32)
    normed_pick = jnp.dot(pick32, normed, precision=highest)
    queries = (
        dot_low(normed_pick.astype(jnp.bfloat16), weights["qkv_weight"][:, :D]) * D ** (-0.5)
        + 0.2 * vector("query_bias")
    ).astype(jnp.bfloat16)
    kv_bias = jnp.concatenate([jnp.zeros((D,), jnp.float32), 0.2 * vector("value_bias")])
    kv_low = (dot_low(normed_low, weights["qkv_weight"][:, D:]) * D ** (-0.5) + kv_bias).astype(
        jnp.bfloat16
    )
    segk = jnp.where(padding_row == 0, segment, -1)[None, :]
    segq = jnp.sum(
        pick32 * segment.astype(jnp.float32)[None, :], 1, keepdims=True
    ).astype(jnp.int32)
    mixed_low = attention(queries, kv_low, segq, segk)
    out_scale = (LONG / D) ** 0.5
    attended = dot_low(mixed_low, weights["out_weight"]) * out_scale + 0.2 * vector("out_bias")
    first, attn_back = jax.vjp(
        layer_norm, normed_pick + attended, vector("attn_gain"), vector("attn_bias")
    )
    first_low = first.astype(jnp.bfloat16)
    hidden_ff = dot_low(first_low, weights["up_weight"]) * D ** (-0.5) + 0.2 * vector("up_bias")
    activated, gelu_ff_back = jax.vjp(gelu_exact, hidden_ff)
    activated_low = activated.astype(jnp.bfloat16)
    branch = dot_low(activated_low, weights["down_weight"]) * FF ** (-0.5) + 0.2 * vector(
        "down_bias"
    )
    second, ffn_back = jax.vjp(layer_norm, first + branch, vector("ffn_gain"), vector("ffn_bias"))
    second_low = second.astype(jnp.bfloat16)
    context = dot_low(second_low, weights["final_weight"]) * D ** (-0.5) + 0.2 * vector(
        "final_bias"
    )
    loss_row, contrast_back = jax.vjp(
        lambda a, b: contrast(a, b, own, weight), context, vector("codebook")
    )
    grad_context, grad_code = contrast_back(jnp.ones_like(loss_row))
    grads = {"codebook": grad_code}
    ctx_low = grad_context.astype(jnp.bfloat16)
    grads["final_weight"] = dot_turn(second_low, ctx_low) * D ** (-0.5)
    grads["final_bias"] = column_sum(ctx_low)
    grad_second = dot_back(ctx_low, weights["final_weight"]) * D ** (-0.5)
    grad_res2, grads["ffn_gain"], grads["ffn_bias"] = ffn_back(grad_second)
    branch_low = grad_res2.astype(jnp.bfloat16)
    grads["down_weight"] = dot_turn(activated_low, branch_low) * FF ** (-0.5)
    grads["down_bias"] = column_sum(branch_low)
    grad_act = dot_back(branch_low, weights["down_weight"]) * FF ** (-0.5)
    ff_grad_low = gelu_ff_back(grad_act)[0].astype(jnp.bfloat16)
    grads["up_weight"] = dot_turn(first_low, ff_grad_low) * D ** (-0.5)
    grads["up_bias"] = column_sum(ff_grad_low)
    grad_first = grad_res2 + dot_back(ff_grad_low, weights["up_weight"]) * D ** (-0.5)
    grad_res1, grads["attn_gain"], grads["attn_bias"] = attn_back(grad_first)
    attended_low = grad_res1.astype(jnp.bfloat16)
    grads["out_weight"] = dot_turn(mixed_low, attended_low) * out_scale
    grads["out_bias"] = column_sum(attended_low)
    grad_mixed = (dot_back(attended_low, weights["out_weight"]) * out_scale).astype(jnp.bfloat16)
    grad_q, grad_k, grad_v = attention_back(queries, kv_low, grad_mixed, segq, segk)
    grads["query_bias"] = column_sum(grad_q)
    grads["value_bias"] = column_sum(grad_v)
    spread_q = dot_turn(pick, grad_q).astype(jnp.bfloat16)
    qkv_grad_low = jnp.concatenate([spread_q, grad_k, grad_v], 1)
    grads["qkv_weight"] = dot_turn(normed_low, qkv_grad_low) * D ** (-0.5)
    grad_normed = lax.dot_general(
        pick32, grad_res1, (((0,), (0,)), ((), ())), precision=highest
    ) + dot_back(qkv_grad_low, weights["qkv_weight"]) * D ** (-0.5)
    grad_embed, grads["enc_gain"], grads["enc_bias"] = enc_back(grad_normed)
    conv_grad_low = gelu_pos_back(grad_embed)[0].astype(jnp.bfloat16)
    grads["pos_bias"] = column_sum(conv_grad_low)
    grad_gap = with_gap(conv_grad_low, edge[0], 16, 1136)
    started = None
    if before_conv is not None:
        grad_gap, started = lax.optimization_barrier((grad_gap, before_conv(grads)))
    input_grad, packed_grad = conv_backward(edge, grad_gap, shifted, packed)
    grads["pos_weight"] = packed_grad
    grad_replaced = grad_embed + input_grad * pos_scale * keep_frame[:, None]
    grads["mask_vector"] = jnp.sum(jnp.where(flagged, grad_replaced, 0.0), 0)
    proj_low = jnp.where(flagged, 0.0, grad_replaced).astype(jnp.bfloat16)
    grads["proj_in"] = dot_turn(hidden_low, proj_low) * FEAT ** (-0.5)
    grads["proj_bias"] = column_sum(proj_low)
    grad_hidden = dot_back(proj_low, weights["proj_in"]) * FEAT ** (-0.5)
    frames_grad, grads["feat_gain"], grads["feat_bias"] = feat_back(grad_hidden)
    return (grads, loss_row, started)


MARGIN = 64
CHUNK = 800 * 1024


def half_pieces(low, high):
    starts, _ = offsets()
    matrices, vectors = [], []
    for key_name, dims in layout():
        if key_name == "pos_weight":
            continue
        first = starts[key_name] // LANE
        count = math.prod(dims) // LANE
        if first >= high or first + count <= low:
            continue
        if len(dims) == 1:
            vectors.append((key_name, first, count))
        else:
            wide = dims[1] // LANE
            begin = max(0, (low - first) // wide // 8 * 8)
            end = min(dims[0], (-(-(high - first) // wide) + 7) // 8 * 8)
            matrices.append((key_name, first, wide, begin, end))
    return matrices, vectors


def chunk_plan(matrices):
    plan = []
    for index, (_, first, wide, begin, end) in enumerate(matrices):
        step = max(8, CHUNK // (wide * LANE * 4) // 8 * 8)
        row = begin
        while row < end:
            count = min(step, end - row)
            plan.append((index, first, wide, row, count))
            row += count
    return plan


def buffer_shapes(matrices):
    return sorted({wide: max(8, CHUNK // (wide * LANE * 4) // 8 * 8) for _, _, wide, _, _ in matrices}.items())


def place_pieces(low, matrices, vectors, refs, vec_refs, stage, buffers, sems):
    plan = chunk_plan(matrices)

    def copy(n):
        index, _, wide, row, count = plan[n]
        slot = n % 2
        return pltpu.make_async_copy(
            refs[index].at[pl.ds(row, count), :],
            buffers[wide].at[slot, pl.ds(0, count), :],
            sems.at[slot],
        )

    copy(0).start()
    for (_, first, count), vec_ref in zip(vectors, vec_refs):
        for k in range(count):
            at = MARGIN + first - low + k
            stage[at : at + 1, :] = vec_ref[:, k * LANE : (k + 1) * LANE]
    for n, (_, first, wide, row, count) in enumerate(plan):
        if n + 1 < len(plan):
            copy(n + 1).start()
        copy(n).wait()
        base = MARGIN + first - low + row * wide
        held = buffers[wide].at[n % 2]

        def body(i, carry, base=base, held=held, wide=wide):
            at = pl.multiple_of(i * 8, 8)
            for k in range(wide):
                stage[pl.ds(base + i * (8 * wide) + k, 8, stride=wide), :] = held[
                    pl.ds(at, 8), k * LANE : (k + 1) * LANE
                ]
            return carry

        lax.fori_loop(0, count // 8, body, 0)


def finish_half(core, shard_rows, padded_rows, stage, mine, other, out_buf, zeros, sems):
    block = shard_rows // 26
    zeros[...] = jnp.zeros_like(zeros)

    def send(j, b, slot, wait):
        def copy(ref):
            return pltpu.make_async_copy(
                out_buf.at[slot],
                ref.at[pl.ds(pl.multiple_of(b * block, 16), block), :],
                sems.at[slot],
            )

        if wait:
            copy(mine).wait()
        else:

            @pl.when(core == j)
            def _():
                copy(mine).start()

            @pl.when(core != j)
            def _():
                copy(other).start()

    for j in range(2):

        def body(i, carry, j=j):
            for slot in range(2):
                b = 2 * i + slot
                if j == 0:

                    @pl.when(i > 0)
                    def _():
                        send(j, b, slot, True)

                else:
                    send(j, b, slot, True)
                at = pl.multiple_of(MARGIN + j * shard_rows + b * block, 16)
                out_buf[slot] = stage[pl.ds(at, block), :].astype(jnp.bfloat16)
                send(j, b, slot, False)
            return carry

        lax.fori_loop(0, 13, body, 0)
    for slot in range(2):
        send(1, 0, slot, True)
    for ref, sem in ((mine, sems.at[0]), (other, sems.at[1])):
        pad = pltpu.make_async_copy(
            zeros, ref.at[pl.ds(shard_rows, padded_rows - shard_rows), :], sem
        )
        pad.start()
        pad.wait()


def half_kernel(core_ref, *refs, low, shard_rows, padded_rows, scale, with_conv):
    high = low + 2 * shard_rows
    matrices, vectors = half_pieces(low, high)
    count = int(with_conv)
    conv_refs, refs = refs[:count], refs[count:]
    mat_refs, refs = refs[: len(matrices)], refs[len(matrices) :]
    vec_refs, refs = refs[: len(vectors)], refs[len(vectors) :]
    mine, other, stage, out_buf, zeros, in_sems, out_sems = refs[:7]
    buffers = {wide: ref for (wide, _), ref in zip(buffer_shapes(matrices), refs[7:])}
    step = pl.program_id(0)

    @pl.when(step == 0)
    def _():
        place_pieces(low, matrices, vectors, mat_refs, vec_refs, stage, buffers, in_sems)
        if low > 0 and not with_conv:
            tail = MARGIN + 2 * shard_rows - 16
            stage[tail : tail + 16, :] = jnp.zeros((16, LANE), jnp.float32)

    if with_conv:
        packed = refs[-1]
        starts, _ = offsets()
        first = MARGIN + starts["pos_weight"] // LANE - low + step * 2304
        for k in range(3):
            packed[k] = (
                conv_refs[0][:, :, k * LANE : (k + 1) * LANE].reshape(GROUPS * WIDTH, LANE) * scale
            )
        for gh in range(2):
            for cb in range(6):
                outs = swap_slots(
                    [
                        load3(packed, (), pl.ds(gh * 384 + 8 * cb + ci, 8, stride=48))
                        for ci in range(8)
                    ]
                )
                for l in range(8):
                    base = first + l * 288 + gh * 144 + 3 * cb
                    for k in range(3):
                        stage[pl.ds(base + k, 8, stride=18), :] = outs[l][k]

    @pl.when(step == pl.num_programs(0) - 1)
    def _():
        finish_half(
            core_ref[0], shard_rows, padded_rows, stage, mine, other, out_buf, zeros, out_sems
        )


def assemble_half(grads, core, low, shard_rows, padded_rows, with_conv):
    high = low + 2 * shard_rows
    matrices, vectors = half_pieces(low, high)
    args, in_specs = [], []
    if with_conv:
        args.append(grads["pos_weight"])
        in_specs.append(pl.BlockSpec((GROUPS, WIDTH, HALF), lambda i, c: (0, i // 2, i % 2)))
    for key_name, _, _, _, _ in matrices:
        args.append(grads[key_name])
        in_specs.append(pl.BlockSpec(memory_space=pl.ANY))
    for key_name, _, count in vectors:
        args.append(grads[key_name].reshape(1, -1))
        in_specs.append(pl.BlockSpec((1, count * LANE), lambda i, c: (0, 0)))
    block = shard_rows // 26
    scratch = [
        pltpu.VMEM((MARGIN + 2 * shard_rows + 192, LANE), jnp.float32),
        pltpu.VMEM((2, block, LANE), jnp.bfloat16),
        pltpu.VMEM((padded_rows - shard_rows, LANE), jnp.bfloat16),
        pltpu.SemaphoreType.DMA((2,)),
        pltpu.SemaphoreType.DMA((2,)),
    ]
    for wide, rows in buffer_shapes(matrices):
        scratch.append(pltpu.VMEM((2, rows, wide * LANE), jnp.float32))
    if with_conv:
        scratch.append(pltpu.VMEM((3, GROUPS * WIDTH, LANE), jnp.float32))
    out = jax.ShapeDtypeStruct((padded_rows, LANE), jnp.bfloat16)
    return pl.pallas_call(
        functools.partial(
            half_kernel,
            low=low,
            shard_rows=shard_rows,
            padded_rows=padded_rows,
            scale=(TAPS * D // GROUPS) ** (-0.5),
            with_conv=with_conv,
        ),
        grid_spec=pltpu.PrefetchScalarGridSpec(
            num_scalar_prefetch=1,
            grid=(16 if with_conv else 1,),
            in_specs=in_specs,
            out_specs=[pl.BlockSpec(memory_space=pl.ANY)] * 2,
            scratch_shapes=scratch,
        ),
        out_shape=[out, out],
        compiler_params=pltpu.CompilerParams(vmem_limit_bytes=VMEM_MAX),
        cost_estimate=pl.CostEstimate(
            flops=10_000_000, bytes_accessed=40_000_000, transcendentals=0
        ),
        name="assemble_conv" if with_conv else "assemble_rest",
    )(core.reshape(1), *args)


CORE_SWAP = [(0, 1), (1, 0), (2, 3), (3, 2)]
Y_SWAP = [(0, 2), (2, 0), (1, 3), (3, 1)]


def pair_half(mine, other):
    arrived = lax.ppermute(other, "shard", CORE_SWAP)
    return (mine.astype(jnp.float32) + arrived.astype(jnp.float32)).astype(jnp.bfloat16)


def reduce_half(pair):
    piece = lax.psum_scatter(pair, "rep", scatter_dimension=0, tiled=True)
    across = lax.ppermute(piece, "shard", Y_SWAP)
    return piece.astype(jnp.float32) + across.astype(jnp.float32)


def split3(value):
    high = value.astype(jnp.bfloat16)
    rest = value - high.astype(jnp.float32)
    mid = rest.astype(jnp.bfloat16)
    low = (rest - mid.astype(jnp.float32)).astype(jnp.bfloat16)
    return [high, mid, low]


def padded_shard(shard_rows):
    return -(-shard_rows // 128) * 128


def start_late(grads, shard_rows):
    core = lax.axis_index("shard") % 2
    return pair_half(
        *assemble_half(grads, core, 2 * shard_rows, shard_rows, padded_shard(shard_rows), False)
    )


def combine_chip(grads, late_pair, loss_local, shard_rows):
    spot = lax.axis_index("shard")
    late = reduce_half(late_pair)
    early = reduce_half(
        pair_half(
            *assemble_half(grads, spot % 2, 0, shard_rows, padded_shard(shard_rows), True)
        )
    )
    own = jnp.where(spot < 2, early, late).astype(jnp.bfloat16)
    terms = jnp.concatenate([jnp.broadcast_to(t, (1, LANE)) for t in split3(loss_local)], 0)
    extra = jnp.pad(terms, ((0, 13), (0, 0)))
    full = lax.all_gather(jnp.concatenate([own, extra], 0), "rep", axis=0, tiled=False)
    piece_rows = own.shape[0]
    loss_rep = jnp.sum(full[:, piece_rows : piece_rows + 3, 0].astype(jnp.float32))
    owned = full[:, :piece_rows].reshape(-1, LANE)[:shard_rows].astype(jnp.float32)
    sums = jnp.stack([jnp.sum(owned * owned), loss_rep])
    sums = jnp.broadcast_to(jnp.pad(sums, (0, 6))[:, None], (8, LANE))
    sums = sums + lax.ppermute(sums, "shard", CORE_SWAP)
    sums = sums + lax.ppermute(sums, "shard", Y_SWAP)
    return owned.reshape(-1), sums[0, 0], sums[1, 0]


def combine_any(grads, loss_local, total_params, shard_count, rep_count):
    _, raw_count = offsets()
    shard_rows = total_params // shard_count // LANE
    piece_rows = -(-shard_rows // (rep_count * 16)) * 16
    flat = dict(grads)
    flat["pos_weight"] = unpack_weights(
        grads["pos_weight"], (TAPS * D // GROUPS) ** (-0.5), jnp.bfloat16
    )
    pieces = [flat[key_name].astype(jnp.bfloat16).reshape(-1, LANE) for key_name, _ in layout()]
    pieces.append(jnp.zeros(((total_params - raw_count) // LANE, LANE), jnp.bfloat16))
    gradient = jnp.concatenate(pieces, 0).reshape(shard_count, shard_rows, LANE)
    gradient = jnp.pad(gradient, ((0, 0), (0, piece_rows * rep_count - shard_rows), (0, 0)))
    reordered = gradient.reshape(shard_count, rep_count, piece_rows, LANE)
    reordered = reordered.transpose(1, 0, 2, 3).reshape(-1, LANE)
    own_piece = lax.psum_scatter(reordered, ("rep", "shard"), scatter_dimension=0, tiled=True)
    own32 = own_piece.astype(jnp.float32)
    square_sum, loss_sum = lax.psum((jnp.sum(own32 * own32), loss_local), ("rep", "shard"))
    owned_grad = lax.all_gather(own_piece, "rep", axis=0, tiled=True)[:shard_rows]
    return owned_grad.reshape(-1).astype(jnp.float32), square_sum, loss_sum


def local(
    frames, segments, padding, masked, distract, targets, params, first_moment, second_moment
):
    shard_count = lax.axis_size("shard")
    rep_count = lax.axis_size("rep")
    full_low = lax.all_gather(params.astype(jnp.bfloat16), "shard", axis=0, tiled=True)
    weights = unpack(full_low)
    starts, raw_count = offsets()
    packed = pack_weights(full_low.reshape(-1, LANE), starts["pos_weight"] // LANE)
    total_params = full_low.shape[0]
    shard_rows = total_params // shard_count // LANE
    fits = (
        (rep_count, shard_count) == (8, 4)
        and frames.shape[0] == 1
        and shard_rows % 416 == 0
        and 4 * shard_rows - raw_count // LANE == 16
        and (starts["pos_weight"] + TAPS * D * WIDTH) // LANE <= 2 * shard_rows
    )
    before_conv = (lambda found: start_late(found, shard_rows)) if fits else None
    grads, loss_local, started = None, jnp.float32(0.0), None
    for row in range(frames.shape[0]):
        inputs = [part[row] for part in (frames, segments, padding, masked, distract, targets)]
        grads_row, loss_row, started = row_step(weights, packed, *inputs, before_conv)
        loss_local = loss_local + loss_row
        grads = grads_row if grads is None else jax.tree.map(jnp.add, grads, grads_row)
    if fits:
        owned_grad, square_sum, loss_sum = combine_chip(grads, started, loss_local, shard_rows)
    else:
        owned_grad, square_sum, loss_sum = combine_any(
            grads, loss_local, total_params, shard_count, rep_count
        )
    clip_limit = 12.0 * math.sqrt(
        masked.shape[1] * frames.shape[0] * rep_count * shard_count / FINAL
    )
    grad_norm = jnp.sqrt(square_sum)
    factor = jnp.minimum(1.0, clip_limit / (grad_norm + 1e-06))
    weight_delta, first_new, second_new = adam_update(
        params, owned_grad * factor, first_moment, second_moment
    )
    return (weight_delta, first_new, second_new, grad_norm, loss_sum)


def solution(mesh):
    in_specs = (
        P(("rep", "shard"), None, None),
        P(("rep", "shard"), None),
        P(("rep", "shard"), None),
        P(("rep", "shard"), None),
        P(("rep", "shard"), None, None),
        P(("rep", "shard"), None),
        P("shard"),
        P("shard"),
        P("shard"),
    )
    out_specs = (P("shard"), P("shard"), P("shard"), P(), P())
    return jax.shard_map(local, mesh=mesh, in_specs=in_specs, out_specs=out_specs, check_vma=False)
```

```python
import functools
import math

import jax
import jax.numpy as jnp
from jax import lax
from jax.experimental import pallas as pl
from jax.experimental.pallas import tpu as pltpu
from jax.sharding import PartitionSpec as P

D = 768
HEADS = 12
HEAD_DIM = 64
FF = 3072
FEAT = 512
TAPS = 128
GROUPS = 16
FINAL = 256
CODES = 640
LONG = 750
ROW = 1024


LANE = 128
WIDTH = D // GROUPS
HALF = D // 2
HALF_GROUPS = 8
GAP = TAPS // 2
TQ = ROW + GAP + 16
VMEM_MAX = 66_000_000
UNROLL = 3
highest = lax.Precision.HIGHEST
inverse_temp = 10.0


def layout():
    return [
        ("feat_gain", (FEAT,)),
        ("feat_bias", (FEAT,)),
        ("proj_in", (FEAT, D)),
        ("proj_bias", (D,)),
        ("mask_vector", (D,)),
        ("pos_weight", (TAPS, GROUPS, WIDTH, WIDTH)),
        ("pos_bias", (D,)),
        ("enc_gain", (D,)),
        ("enc_bias", (D,)),
        ("qkv_weight", (D, 3 * D)),
        ("query_bias", (D,)),
        ("value_bias", (D,)),
        ("out_weight", (D, D)),
        ("out_bias", (D,)),
        ("attn_gain", (D,)),
        ("attn_bias", (D,)),
        ("up_weight", (D, FF)),
        ("up_bias", (FF,)),
        ("down_weight", (FF, D)),
        ("down_bias", (D,)),
        ("ffn_gain", (D,)),
        ("ffn_bias", (D,)),
        ("final_weight", (D, FINAL)),
        ("final_bias", (FINAL,)),
        ("codebook", (CODES, FINAL)),
    ]


class Bag(dict):
    __getattr__ = dict.__getitem__
    __setattr__ = dict.__setitem__


def offsets():
    result = Bag()
    offset = 0
    for key_name, dims in layout():
        result[key_name] = offset
        offset += math.prod(dims)
    return result, offset


def unpack(flat):
    starts, _ = offsets()
    result = Bag()
    for key_name, dims in layout():
        if key_name != "pos_weight":
            start = starts[key_name]
            result[key_name] = flat[start : start + math.prod(dims)].reshape(dims)
    return result


def layer_norm(values, gain_raw, bias_raw):
    centered = values - jnp.mean(values, -1, keepdims=True)
    scale_inv = lax.rsqrt(jnp.mean(centered * centered, -1, keepdims=True) + 1e-05)
    return centered * scale_inv * (1.0 + 0.2 * gain_raw) + 0.2 * bias_raw


def gelu_exact(values):
    return jax.nn.gelu(values, approximate=False)


def adam_update(weight_old, grad_scaled, first_old, second_old):
    first_new = 0.5 * first_old + 0.5 * grad_scaled
    second_new = 0.5 * second_old + 0.5 * grad_scaled * grad_scaled
    first_hat = first_new / (1.0 - 0.5**4)
    second_hat = second_new / (1.0 - 0.5**4)
    weight_delta = -0.1 * (first_hat / (jnp.sqrt(second_hat) + 1e-08) + 0.01 * weight_old)
    return (weight_delta, first_new, second_new)


def swap_plan(bit):
    plans = []
    for keep in (0, 1):
        tiles = []
        for v in range(3):
            found = {}
            for lane in range(LANE):
                at = v * LANE + lane
                high = 1 if (at // WIDTH) & bit else 0
                source = at + WIDTH * bit * (keep - high)
                key = (high, source // LANE, (lane - source) % LANE)
                runs = found.setdefault(key, [])
                if runs and runs[-1][1] == lane:
                    runs[-1][1] = lane + 1
                else:
                    runs.append([lane, lane + 1])
            tiles.append(sorted(found.items(), key=lambda e: -sum(h - l for l, h in e[1])))
        plans.append(tiles)
    return plans


PLANS = {bit: swap_plan(bit) for bit in (4, 2, 1)}


def lane_runs(shape, runs):
    lane = lax.broadcasted_iota(jnp.int32, shape, 1)
    result = None
    for low, high in runs:
        part = None
        if low > 0:
            part = lane >= low
        if high < LANE:
            part = lane < high if part is None else part & (lane < high)
        result = part if result is None else result | part
    return result


def swap_half(pair, bit, keep):
    turned = {}

    def source(key):
        array, tile, turn = key
        if key not in turned:
            value = pair[array][tile]
            turned[key] = pltpu.roll(value, turn, 1) if turn else value
        return turned[key]

    result = []
    for entries in PLANS[bit][keep]:
        value = source(entries[0][0])
        for key, runs in entries[1:]:
            value = jnp.where(lane_runs(value.shape, runs), source(key), value)
        result.append(value)
    return result


def swap_slots(arrays):
    arrays = list(arrays)
    for bit in (4, 2, 1):
        done = list(arrays)
        for i in range(8):
            if i & bit == 0:
                pair = (arrays[i], arrays[i | bit])
                done[i] = swap_half(pair, bit, 0)
                done[i | bit] = swap_half(pair, bit, 1)
        arrays = done
    return arrays


def fold_slots(near, far, near_next, far_next, bit):
    kept = swap_half((near, far), bit, 0)
    moved = swap_half((near_next, far_next), bit, 1)
    return [a + b for a, b in zip(kept, moved)]


def repeat(first, last, body):
    count = last - first
    group = next(n for n in (UNROLL, UNROLL - 1, 2, 1) if n > 0 and count % n == 0)

    def several(i, carry):
        for n in range(group):
            body(first + i * group + n, carry)
        return carry

    lax.fori_loop(0, count // group, several, 0)


def load3(ref, lead, rows):
    return [ref[lead + (k, rows)] for k in range(3)]


def store3(ref, lead, rows, value):
    for k in range(3):
        ref[lead + (k, rows)] = value[k]


def weight_pack_kernel(w_ref, o_ref, flat, packed, *, lead):
    flat[...] = w_ref[...].astype(jnp.float32)
    for gh in range(2):
        for cb in range(6):
            taps = []
            for l in range(8):
                base = lead + l * 288 + gh * 144 + 3 * cb
                taps.append([flat[pl.ds(base + k, 8, stride=18), :] for k in range(3)])
            outs = swap_slots(taps)
            for ci in range(8):
                store3(packed, (), pl.ds(gh * 384 + 8 * cb + ci, 8, stride=48), outs[ci])
    for k in range(3):
        o_ref[:, :, k * LANE : (k + 1) * LANE] = (
            packed[k].reshape(GROUPS, WIDTH, LANE).astype(jnp.bfloat16)
        )


def pack_weights(flat_rows, first_row):
    lead = first_row % 16
    start = first_row - lead
    return pl.pallas_call(
        functools.partial(weight_pack_kernel, lead=lead),
        grid=(16,),
        in_specs=[
            pl.BlockSpec((pl.Element(2304 + 16), pl.Element(LANE)), lambda i: (pl.multiple_of(start + 2304 * i, 16), 0))
        ],
        out_specs=pl.BlockSpec((GROUPS, WIDTH, HALF), lambda i: (0, i // 2, i % 2)),
        out_shape=jax.ShapeDtypeStruct((GROUPS, HALF, D), jnp.bfloat16),
        scratch_shapes=[
            pltpu.VMEM((2304 + 16, LANE), jnp.float32),
            pltpu.VMEM((3, GROUPS * WIDTH, LANE), jnp.float32),
        ],
        compiler_params=pltpu.CompilerParams(vmem_limit_bytes=VMEM_MAX),
    )(flat_rows)


def weight_unpack_kernel(w_ref, o_ref, flat, packed, *, scale):
    for k in range(3):
        packed[k] = (
            w_ref[:, :, k * LANE : (k + 1) * LANE].reshape(GROUPS * WIDTH, LANE) * scale
        )
    for gh in range(2):
        for cb in range(6):
            outs = swap_slots(
                [
                    load3(packed, (), pl.ds(gh * 384 + 8 * cb + ci, 8, stride=48))
                    for ci in range(8)
                ]
            )
            for l in range(8):
                base = l * 288 + gh * 144 + 3 * cb
                for k in range(3):
                    flat[pl.ds(base + k, 8, stride=18), :] = outs[l][k]
    o_ref[...] = flat[...].astype(o_ref.dtype)


def unpack_weights(packed, scale, dtype):
    return pl.pallas_call(
        functools.partial(weight_unpack_kernel, scale=scale),
        grid=(16,),
        in_specs=[pl.BlockSpec((GROUPS, WIDTH, HALF), lambda i: (0, i // 2, i % 2))],
        out_specs=pl.BlockSpec((2304, LANE), lambda i: (i, 0)),
        out_shape=jax.ShapeDtypeStruct((16 * 2304, LANE), dtype),
        scratch_shapes=[
            pltpu.VMEM((2304, LANE), jnp.float32),
            pltpu.VMEM((3, GROUPS * WIDTH, LANE), jnp.float32),
        ],
        compiler_params=pltpu.CompilerParams(vmem_limit_bytes=VMEM_MAX),
    )(packed)


def rows_at(start, count):
    return pl.ds(start, count)


def conv_fwd_kernel(edge_ref, x_ref, w_ref, y_ref, xs_ref, xs_all, zs, v_all, c1, d1, e1):
    g = pl.program_id(1)

    @pl.when(g == 0)
    def _():
        def build(i, carry):
            t0 = pl.multiple_of(i * 16, 16)
            outs = swap_slots(
                [
                    [x_ref[pl.ds(t0 + 16 * a, 16), k * LANE : (k + 1) * LANE] for k in range(3)]
                    for a in range(8)
                ]
            )
            for q in range(8):
                for k in range(3):
                    xs_all[q, pl.ds(t0, 16), k * LANE : (k + 1) * LANE] = outs[q][k]
            return carry

        repeat(0, TQ // 16, build)

    xs_ref[0] = xs_all[g]
    for c in range(3):
        z = jnp.dot(
            xs_all[g, c * 368 : (c + 1) * 368, :],
            w_ref[0],
            preferred_element_type=jnp.float32,
        )
        for k in range(6):
            zs[k, c * 368 : (c + 1) * 368, :] = z[:, k * LANE : (k + 1) * LANE]

    def add_high(i, carry):
        t0 = pl.multiple_of(i * 48, 8)
        for k in range(3):
            v_all[g, k, pl.ds(t0, 48), :] = (
                zs[k, pl.ds(t0, 48), :] + zs[k + 3, pl.ds(t0 + 8, 48), :]
            )
        return carry

    repeat(0, TQ // 48, add_high)

    @pl.when(g == HALF_GROUPS - 1)
    def _():
        def fold(src, dst, count, bit):
            def body(i, carry):
                t0 = pl.multiple_of(i * 16, 16)
                for p in range(count):
                    value = fold_slots(
                        load3(src, (p,), pl.ds(t0, 16)),
                        load3(src, (p + count,), pl.ds(t0, 16)),
                        load3(src, (p,), pl.ds(t0 + bit, 16)),
                        load3(src, (p + count,), pl.ds(t0 + bit, 16)),
                        bit,
                    )
                    store3(dst, (p,), pl.ds(t0, 16), value)
                return carry

            return body

        repeat(0, TQ // 16, fold(v_all, c1, 4, 4))
        repeat(0, TQ // 16, fold(c1, d1, 2, 2))
        repeat(0, TQ // 16, fold(d1, e1, 1, 1))
        edge = edge_ref[0]

        def place(i, carry):
            t0 = pl.multiple_of(i * 16, 16)
            row = t0 + lax.broadcasted_iota(jnp.int32, (16, LANE), 0)
            for k in range(3):
                y_ref[pl.ds(t0, 16), k * LANE : (k + 1) * LANE] = jnp.where(
                    row < edge, e1[0, k, pl.ds(t0, 16), :], e1[0, k, pl.ds(t0 + GAP, 16), :]
                )
            return carry

        repeat(0, ROW // 16, place)


def conv_forward(edge, x_gap, packed):
    rows = TQ + 16
    return pl.pallas_call(
        conv_fwd_kernel,
        grid_spec=pltpu.PrefetchScalarGridSpec(
            num_scalar_prefetch=1,
            grid=(2, HALF_GROUPS),
            in_specs=[
                pl.BlockSpec((ROW + 3 * GAP, HALF), lambda h, g, e: (0, h)),
                pl.BlockSpec((1, HALF, D), lambda h, g, e: (h * HALF_GROUPS + g, 0, 0)),
            ],
            out_specs=[
                pl.BlockSpec((ROW, HALF), lambda h, g, e: (0, h)),
                pl.BlockSpec((1, TQ, HALF), lambda h, g, e: (h * HALF_GROUPS + g, 0, 0)),
            ],
            scratch_shapes=[
                pltpu.VMEM((HALF_GROUPS, TQ, HALF), jnp.bfloat16),
                pltpu.VMEM((6, rows, LANE), jnp.float32),
                pltpu.VMEM((8, 3, rows, LANE), jnp.float32),
                pltpu.VMEM((4, 3, rows, LANE), jnp.float32),
                pltpu.VMEM((2, 3, rows, LANE), jnp.float32),
                pltpu.VMEM((1, 3, rows, LANE), jnp.float32),
            ],
        ),
        out_shape=[
            jax.ShapeDtypeStruct((ROW, D), jnp.float32),
            jax.ShapeDtypeStruct((GROUPS, TQ, HALF), jnp.bfloat16),
        ],
        compiler_params=pltpu.CompilerParams(vmem_limit_bytes=VMEM_MAX),
        cost_estimate=pl.CostEstimate(flops=60_000_000_000, bytes_accessed=60_000_000, transcendentals=0),
    )(edge, x_gap, packed)


BACK = ROW + 3 * GAP


def conv_bwd_kernel(
    edge_ref, dy_ref, xs_ref, w_ref, dx_ref, dw_ref, dys, dl, dz, dxs, d1, e1
):
    g = pl.program_id(1)

    @pl.when(g == 0)
    def _():
        def spread(i, carry):
            t0 = pl.multiple_of(i * 16, 16)
            part = dy_ref[pl.ds(t0, 16), :].astype(jnp.float32)
            store3(dys, (), pl.ds(t0, 16), [part[:, k * LANE : (k + 1) * LANE] for k in range(3)])
            return carry

        repeat(0, 1136 // 16, spread)

        def build(i, carry):
            u0 = pl.multiple_of(i * 16, 16)
            outs = swap_slots([load3(dys, (), pl.ds(u0 + 8 - l, 16)) for l in range(8)])
            for q in range(8):
                store3(dl, (q,), pl.ds(u0, 16), outs[q])
            return carry

        repeat(0, 1120 // 16, build)
        zero = jnp.zeros((16, LANE), jnp.float32)

        def clear(i, carry):
            for q in range(8):
                for k in range(3):
                    dxs[q, k, pl.ds(pl.multiple_of(i * 16, 16), 16), :] = zero
            return carry

        repeat(0, GAP // 16, clear)
        repeat((GAP + TQ) // 16, BACK // 16, clear)

    def pack(i, carry):
        t0 = pl.multiple_of(i * 16, 16)
        for k in range(3):
            dz[pl.ds(t0, 16), k * LANE : (k + 1) * LANE] = dl[g, k, pl.ds(t0 + 8, 16), :].astype(
                jnp.bfloat16
            )
            dz[pl.ds(t0, 16), HALF + k * LANE : HALF + (k + 1) * LANE] = dl[
                g, k, pl.ds(t0, 16), :
            ].astype(jnp.bfloat16)
        return carry

    repeat(0, TQ // 16, pack)
    dw_ref[0] = lax.dot_general(
        xs_ref[0], dz[...], (((0,), (0,)), ((), ())), preferred_element_type=jnp.float32
    )
    for c in range(3):
        back = lax.dot_general(
            dz[c * 368 : (c + 1) * 368, :],
            w_ref[0],
            (((1,), (1,)), ((), ())),
            preferred_element_type=jnp.float32,
        )
        for k in range(3):
            dxs[g, k, GAP + c * 368 : GAP + (c + 1) * 368, :] = back[:, k * LANE : (k + 1) * LANE]

    @pl.when(g == HALF_GROUPS - 1)
    def _():
        def fold(src, dst, count, bit, first):
            def body(i, carry):
                t0 = pl.multiple_of(i * 16, 16)
                for p in range(count):
                    value = fold_slots(
                        load3(src, (p,), pl.ds(t0, 16)),
                        load3(src, (p + count,), pl.ds(t0, 16)),
                        load3(src, (p,), pl.ds(t0 - 16 * bit, 16)),
                        load3(src, (p + count,), pl.ds(t0 - 16 * bit, 16)),
                        bit,
                    )
                    store3(dst, (p,), pl.ds(t0, 16), value)
                return carry

            repeat(first // 16, BACK // 16, body)

        fold(dxs, dl, 4, 4, 64)
        fold(dl, d1, 2, 2, 96)
        fold(d1, e1, 1, 1, 112)
        edge = edge_ref[0]

        def place(i, carry):
            t0 = pl.multiple_of(i * 16, 16)
            row = t0 + lax.broadcasted_iota(jnp.int32, (16, LANE), 0)
            for k in range(3):
                dx_ref[pl.ds(t0, 16), k * LANE : (k + 1) * LANE] = jnp.where(
                    row < edge,
                    e1[0, k, pl.ds(t0 + 2 * GAP, 16), :],
                    e1[0, k, pl.ds(t0 + 3 * GAP, 16), :],
                )
            return carry

        repeat(0, ROW // 16, place)


def conv_backward(edge, dy_gap, shifted, packed):
    return pl.pallas_call(
        conv_bwd_kernel,
        grid_spec=pltpu.PrefetchScalarGridSpec(
            num_scalar_prefetch=1,
            grid=(2, HALF_GROUPS),
            in_specs=[
                pl.BlockSpec((1136, HALF), lambda h, g, e: (0, h)),
                pl.BlockSpec((1, TQ, HALF), lambda h, g, e: (h * HALF_GROUPS + g, 0, 0)),
                pl.BlockSpec((1, HALF, D), lambda h, g, e: (h * HALF_GROUPS + g, 0, 0)),
            ],
            out_specs=[
                pl.BlockSpec((ROW, HALF), lambda h, g, e: (0, h)),
                pl.BlockSpec((1, HALF, D), lambda h, g, e: (h * HALF_GROUPS + g, 0, 0)),
            ],
            scratch_shapes=[
                pltpu.VMEM((3, 1136, LANE), jnp.float32),
                pltpu.VMEM((8, 3, BACK, LANE), jnp.float32),
                pltpu.VMEM((TQ, D), jnp.bfloat16),
                pltpu.VMEM((8, 3, BACK, LANE), jnp.float32),
                pltpu.VMEM((2, 3, BACK, LANE), jnp.float32),
                pltpu.VMEM((1, 3, BACK, LANE), jnp.float32),
            ],
        ),
        out_shape=[
            jax.ShapeDtypeStruct((ROW, D), jnp.float32),
            jax.ShapeDtypeStruct((GROUPS, HALF, D), jnp.float32),
        ],
        compiler_params=pltpu.CompilerParams(vmem_limit_bytes=VMEM_MAX),
        cost_estimate=pl.CostEstimate(flops=90_000_000_000, bytes_accessed=80_000_000, transcendentals=0),
    )(edge, dy_gap, shifted, packed)


def with_gap(values, edge, before, total):
    near = jnp.pad(values, ((before, total - ROW - before), (0, 0)))
    far = jnp.pad(values, ((before + GAP, total - ROW - before - GAP), (0, 0)))
    row = lax.broadcasted_iota(jnp.int32, (total, 1), 0) - before
    zero = jnp.zeros((), values.dtype)
    return jnp.where(row < edge, near, jnp.where(row >= edge + GAP, far, zero))


def head_scores(q_ref, k_ref, segq_ref, segk_ref, sub, rows):
    cols = slice(sub * HEAD_DIM, (sub + 1) * HEAD_DIM)
    scores = lax.dot_general(
        q_ref[rows, cols], k_ref[:, cols], (((1,), (1,)), ((), ())),
        preferred_element_type=jnp.float32,
    ) * HEAD_DIM ** (-0.5)
    allowed = segq_ref[rows, :] == segk_ref[...]
    scores = jnp.where(allowed, scores, -1e30)
    power = jnp.exp(scores - jnp.max(scores, -1, keepdims=True))
    return power * (1.0 / jnp.sum(power, -1, keepdims=True))


def attn_fwd_kernel(q_ref, k_ref, v_ref, segq_ref, segk_ref, o_ref):
    for block in range(q_ref.shape[0] // LANE):
        rows = slice(block * LANE, (block + 1) * LANE)
        parts = []
        for sub in range(2):
            probs = head_scores(q_ref, k_ref, segq_ref, segk_ref, sub, rows)
            parts.append(
                jnp.dot(
                    probs.astype(jnp.bfloat16),
                    v_ref[:, sub * HEAD_DIM : (sub + 1) * HEAD_DIM],
                    preferred_element_type=jnp.float32,
                )
            )
        o_ref[rows, :] = jnp.concatenate(parts, 1).astype(jnp.bfloat16)


def attn_bwd_kernel(
    q_ref, k_ref, v_ref, g_ref, segq_ref, segk_ref, dq_ref, dk_ref, dv_ref, probs_low, ds_low
):
    for sub in range(2):
        cols = slice(sub * HEAD_DIM, (sub + 1) * HEAD_DIM)
        for block in range(q_ref.shape[0] // LANE):
            rows = slice(block * LANE, (block + 1) * LANE)
            probs = head_scores(q_ref, k_ref, segq_ref, segk_ref, sub, rows)
            probs_low[rows, :] = probs.astype(jnp.bfloat16)
            grad_probs = lax.dot_general(
                g_ref[rows, cols], v_ref[:, cols], (((1,), (1,)), ((), ())),
                preferred_element_type=jnp.float32,
            )
            total = jnp.sum(probs * grad_probs, -1, keepdims=True)
            ds_low[rows, :] = (probs * (grad_probs - total)).astype(jnp.bfloat16)
        scale = HEAD_DIM ** (-0.5)
        turn = (((0,), (0,)), ((), ()))
        dv_ref[:, cols] = lax.dot_general(
            probs_low[...], g_ref[:, cols], turn, preferred_element_type=jnp.float32
        ).astype(jnp.bfloat16)
        dk_ref[:, cols] = (
            lax.dot_general(
                ds_low[...], q_ref[:, cols], turn, preferred_element_type=jnp.float32
            )
            * scale
        ).astype(jnp.bfloat16)
        dq_ref[:, cols] = (
            jnp.dot(ds_low[...], k_ref[:, cols], preferred_element_type=jnp.float32) * scale
        ).astype(jnp.bfloat16)


def attention(queries, kv, segq, segk):
    count = queries.shape[0]
    pairs = HEADS // 2
    return pl.pallas_call(
        attn_fwd_kernel,
        grid=(pairs,),
        in_specs=[
            pl.BlockSpec((count, LANE), lambda h: (0, h)),
            pl.BlockSpec((ROW, LANE), lambda h: (0, h)),
            pl.BlockSpec((ROW, LANE), lambda h: (0, pairs + h)),
            pl.BlockSpec((count, 1), lambda h: (0, 0)),
            pl.BlockSpec((1, ROW), lambda h: (0, 0)),
        ],
        out_specs=pl.BlockSpec((count, LANE), lambda h: (0, h)),
        out_shape=jax.ShapeDtypeStruct((count, D), jnp.bfloat16),
        compiler_params=pltpu.CompilerParams(vmem_limit_bytes=VMEM_MAX // 2),
    )(queries, kv, kv, segq, segk)


def attention_back(queries, kv, grad, segq, segk):
    count = queries.shape[0]
    pairs = HEADS // 2
    return pl.pallas_call(
        attn_bwd_kernel,
        grid=(pairs,),
        in_specs=[
            pl.BlockSpec((count, LANE), lambda h: (0, h)),
            pl.BlockSpec((ROW, LANE), lambda h: (0, h)),
            pl.BlockSpec((ROW, LANE), lambda h: (0, pairs + h)),
            pl.BlockSpec((count, LANE), lambda h: (0, h)),
            pl.BlockSpec((count, 1), lambda h: (0, 0)),
            pl.BlockSpec((1, ROW), lambda h: (0, 0)),
        ],
        out_specs=[
            pl.BlockSpec((count, LANE), lambda h: (0, h)),
            pl.BlockSpec((ROW, LANE), lambda h: (0, h)),
            pl.BlockSpec((ROW, LANE), lambda h: (0, h)),
        ],
        out_shape=[
            jax.ShapeDtypeStruct((count, D), jnp.bfloat16),
            jax.ShapeDtypeStruct((ROW, D), jnp.bfloat16),
            jax.ShapeDtypeStruct((ROW, D), jnp.bfloat16),
        ],
        scratch_shapes=[
            pltpu.VMEM((count, ROW), jnp.bfloat16),
            pltpu.VMEM((count, ROW), jnp.bfloat16),
        ],
        compiler_params=pltpu.CompilerParams(vmem_limit_bytes=VMEM_MAX // 2),
    )(queries, kv, kv, grad, segq, segk)


def dot_low(left, right):
    return jnp.dot(left, right, preferred_element_type=jnp.float32)


def dot_turn(left, right):
    return lax.dot_general(
        left, right, (((0,), (0,)), ((), ())), preferred_element_type=jnp.float32
    )


def dot_back(left, right):
    return lax.dot_general(
        left, right, (((1,), (1,)), ((), ())), preferred_element_type=jnp.float32
    )


def contrast_counts(masked_row, distract_row, target_row):
    frame = lax.broadcasted_iota(jnp.int32, (1, 1, ROW), 2)
    seen = jnp.sum((distract_row[:, :, None] == frame).astype(jnp.float32), 1)
    code = lax.broadcasted_iota(jnp.int32, (ROW, CODES), 1)
    is_code = (target_row[:, None] == code).astype(jnp.bfloat16)
    counts = dot_low(seen.astype(jnp.bfloat16), is_code)
    pick = (masked_row[:, None] == lax.broadcasted_iota(jnp.int32, (1, ROW), 1)).astype(
        jnp.bfloat16
    )
    own = dot_low(pick, is_code)
    return pick, own, jnp.where(own > 0, 1.0, counts)


def contrast(picked, codebook, own, weight):
    picked_unit = picked * lax.rsqrt(jnp.sum(picked * picked, -1, keepdims=True) + 1e-06)
    code_unit = codebook * lax.rsqrt(jnp.sum(codebook * codebook, -1, keepdims=True) + 1e-06)
    logits = inverse_temp * jnp.dot(
        picked_unit, code_unit.T, precision=highest, preferred_element_type=jnp.float32
    )
    logits = jnp.where(weight > 0, logits, -1e30)
    top = lax.stop_gradient(jnp.max(logits, -1, keepdims=True))
    total = jnp.sum(weight * jnp.exp(logits - top), -1)
    return jnp.sum(top[:, 0] + jnp.log(total) - jnp.sum(own * logits, -1))


def column_sum(rounded):
    return 0.2 * jnp.sum(rounded.astype(jnp.float32), 0)


def row_step(
    weights,
    packed,
    frames_row,
    segment,
    padding_row,
    masked_row,
    distract_row,
    target_row,
    before_conv=None,
):
    vector = Bag((name, part.astype(jnp.float32)) for name, part in weights.items())
    pick, own, weight = contrast_counts(masked_row, distract_row, target_row)
    edge = jnp.sum((segment == 0).astype(jnp.int32)).reshape(1)
    keep_frame = (1 - padding_row).astype(jnp.float32)
    hidden_in, feat_back = jax.vjp(
        layer_norm, frames_row.astype(jnp.float32), vector.feat_gain, vector.feat_bias
    )
    hidden_low = hidden_in.astype(jnp.bfloat16)
    projected = dot_low(hidden_low, weights.proj_in) * FEAT ** (-0.5) + 0.2 * vector.proj_bias
    flagged = jnp.any(
        masked_row[None, :] == lax.broadcasted_iota(jnp.int32, (ROW, 1), 0), 1, keepdims=True
    )
    replaced = jnp.where(flagged, vector.mask_vector[None, :], projected)
    conv_in = (replaced * keep_frame[:, None]).astype(jnp.bfloat16)
    pos_scale = (TAPS * D // GROUPS) ** (-0.5)
    conv_sum, shifted = conv_forward(edge, with_gap(conv_in, edge[0], GAP, ROW + 3 * GAP), packed)
    conv_out = conv_sum * pos_scale + 0.2 * vector.pos_bias
    activated_pos, gelu_pos_back = jax.vjp(gelu_exact, conv_out)
    normed, enc_back = jax.vjp(
        layer_norm, replaced + activated_pos, vector.enc_gain, vector.enc_bias
    )
    normed_low = normed.astype(jnp.bfloat16)
    pick32 = pick.astype(jnp.float32)
    normed_pick = jnp.dot(pick32, normed, precision=highest)
    queries = (
        dot_low(normed_pick.astype(jnp.bfloat16), weights.qkv_weight[:, :D]) * D ** (-0.5)
        + 0.2 * vector.query_bias
    ).astype(jnp.bfloat16)
    kv_bias = jnp.concatenate([jnp.zeros((D,), jnp.float32), 0.2 * vector.value_bias])
    kv_low = (dot_low(normed_low, weights.qkv_weight[:, D:]) * D ** (-0.5) + kv_bias).astype(
        jnp.bfloat16
    )
    segk = jnp.where(padding_row == 0, segment, -1)[None, :]
    segq = jnp.sum(
        pick32 * segment.astype(jnp.float32)[None, :], 1, keepdims=True
    ).astype(jnp.int32)
    mixed_low = attention(queries, kv_low, segq, segk)
    out_scale = (LONG / D) ** 0.5
    attended = dot_low(mixed_low, weights.out_weight) * out_scale + 0.2 * vector.out_bias
    first, attn_back = jax.vjp(
        layer_norm, normed_pick + attended, vector.attn_gain, vector.attn_bias
    )
    first_low = first.astype(jnp.bfloat16)
    hidden_ff = dot_low(first_low, weights.up_weight) * D ** (-0.5) + 0.2 * vector.up_bias
    activated, gelu_ff_back = jax.vjp(gelu_exact, hidden_ff)
    activated_low = activated.astype(jnp.bfloat16)
    branch = dot_low(activated_low, weights.down_weight) * FF ** (-0.5) + 0.2 * vector.down_bias
    second, ffn_back = jax.vjp(layer_norm, first + branch, vector.ffn_gain, vector.ffn_bias)
    second_low = second.astype(jnp.bfloat16)
    context = dot_low(second_low, weights.final_weight) * D ** (-0.5) + 0.2 * vector.final_bias
    loss_row, contrast_back = jax.vjp(
        lambda a, b: contrast(a, b, own, weight), context, vector.codebook
    )
    grad_context, grad_code = contrast_back(jnp.ones_like(loss_row))
    grads = Bag(codebook=grad_code)
    ctx_low = grad_context.astype(jnp.bfloat16)
    grads.final_weight = dot_turn(second_low, ctx_low) * D ** (-0.5)
    grads.final_bias = column_sum(ctx_low)
    grad_second = dot_back(ctx_low, weights.final_weight) * D ** (-0.5)
    grad_res2, grads.ffn_gain, grads.ffn_bias = ffn_back(grad_second)
    branch_low = grad_res2.astype(jnp.bfloat16)
    grads.down_weight = dot_turn(activated_low, branch_low) * FF ** (-0.5)
    grads.down_bias = column_sum(branch_low)
    grad_act = dot_back(branch_low, weights.down_weight) * FF ** (-0.5)
    ff_grad_low = gelu_ff_back(grad_act)[0].astype(jnp.bfloat16)
    grads.up_weight = dot_turn(first_low, ff_grad_low) * D ** (-0.5)
    grads.up_bias = column_sum(ff_grad_low)
    grad_first = grad_res2 + dot_back(ff_grad_low, weights.up_weight) * D ** (-0.5)
    grad_res1, grads.attn_gain, grads.attn_bias = attn_back(grad_first)
    attended_low = grad_res1.astype(jnp.bfloat16)
    grads.out_weight = dot_turn(mixed_low, attended_low) * out_scale
    grads.out_bias = column_sum(attended_low)
    grad_mixed = (dot_back(attended_low, weights.out_weight) * out_scale).astype(jnp.bfloat16)
    grad_q, grad_k, grad_v = attention_back(queries, kv_low, grad_mixed, segq, segk)
    grads.query_bias = column_sum(grad_q)
    grads.value_bias = column_sum(grad_v)
    spread_q = dot_turn(pick, grad_q).astype(jnp.bfloat16)
    qkv_grad_low = jnp.concatenate([spread_q, grad_k, grad_v], 1)
    grads.qkv_weight = dot_turn(normed_low, qkv_grad_low) * D ** (-0.5)
    grad_normed = lax.dot_general(
        pick32, grad_res1, (((0,), (0,)), ((), ())), precision=highest
    ) + dot_back(qkv_grad_low, weights.qkv_weight) * D ** (-0.5)
    grad_embed, grads.enc_gain, grads.enc_bias = enc_back(grad_normed)
    conv_grad_low = gelu_pos_back(grad_embed)[0].astype(jnp.bfloat16)
    grads.pos_bias = column_sum(conv_grad_low)
    grad_gap = with_gap(conv_grad_low, edge[0], 16, 1136)
    started = None
    if before_conv is not None:
        grad_gap, started = lax.optimization_barrier((grad_gap, before_conv(grads)))
    input_grad, packed_grad = conv_backward(edge, grad_gap, shifted, packed)
    grads.pos_weight = packed_grad
    grad_replaced = grad_embed + input_grad * pos_scale * keep_frame[:, None]
    grads.mask_vector = jnp.sum(jnp.where(flagged, grad_replaced, 0.0), 0)
    proj_low = jnp.where(flagged, 0.0, grad_replaced).astype(jnp.bfloat16)
    grads.proj_in = dot_turn(hidden_low, proj_low) * FEAT ** (-0.5)
    grads.proj_bias = column_sum(proj_low)
    grad_hidden = dot_back(proj_low, weights.proj_in) * FEAT ** (-0.5)
    frames_grad, grads.feat_gain, grads.feat_bias = feat_back(grad_hidden)
    return (dict(grads), loss_row, started)


MARGIN = 64
CHUNK = 800 * 1024


def half_pieces(low, high):
    starts, _ = offsets()
    matrices, vectors = [], []
    for key_name, dims in layout():
        if key_name == "pos_weight":
            continue
        first = starts[key_name] // LANE
        count = math.prod(dims) // LANE
        if first >= high or first + count <= low:
            continue
        if len(dims) == 1:
            vectors.append((key_name, first, count))
        else:
            wide = dims[1] // LANE
            begin = max(0, (low - first) // wide // 8 * 8)
            end = min(dims[0], (-(-(high - first) // wide) + 7) // 8 * 8)
            matrices.append((key_name, first, wide, begin, end))
    return matrices, vectors


def chunk_plan(matrices):
    plan = []
    for index, (_, first, wide, begin, end) in enumerate(matrices):
        step = max(8, CHUNK // (wide * LANE * 4) // 8 * 8)
        row = begin
        while row < end:
            count = min(step, end - row)
            plan.append((index, first, wide, row, count))
            row += count
    return plan


def buffer_shapes(matrices):
    return sorted({wide: max(8, CHUNK // (wide * LANE * 4) // 8 * 8) for _, _, wide, _, _ in matrices}.items())


def place_pieces(low, matrices, vectors, refs, vec_refs, stage, buffers, sems):
    plan = chunk_plan(matrices)

    def copy(n):
        index, _, wide, row, count = plan[n]
        slot = n % 2
        return pltpu.make_async_copy(
            refs[index].at[pl.ds(row, count), :],
            buffers[wide].at[slot, pl.ds(0, count), :],
            sems.at[slot],
        )

    copy(0).start()
    for (_, first, count), vec_ref in zip(vectors, vec_refs):
        for k in range(count):
            at = MARGIN + first - low + k
            stage[at : at + 1, :] = vec_ref[:, k * LANE : (k + 1) * LANE]
    for n, (_, first, wide, row, count) in enumerate(plan):
        if n + 1 < len(plan):
            copy(n + 1).start()
        copy(n).wait()
        base = MARGIN + first - low + row * wide
        held = buffers[wide].at[n % 2]

        def body(i, carry, base=base, held=held, wide=wide):
            at = pl.multiple_of(i * 8, 8)
            for k in range(wide):
                stage[pl.ds(base + i * (8 * wide) + k, 8, stride=wide), :] = held[
                    pl.ds(at, 8), k * LANE : (k + 1) * LANE
                ]
            return carry

        repeat(0, count // 8, body)


def finish_half(core, shard_rows, padded_rows, stage, mine, other, out_buf, zeros, sems):
    block = shard_rows // 26
    zeros[...] = jnp.zeros_like(zeros)

    def send(j, b, slot, wait):
        def copy(ref):
            return pltpu.make_async_copy(
                out_buf.at[slot],
                ref.at[pl.ds(pl.multiple_of(b * block, 16), block), :],
                sems.at[slot],
            )

        if wait:
            copy(mine).wait()
        else:

            @pl.when(core == j)
            def _():
                copy(mine).start()

            @pl.when(core != j)
            def _():
                copy(other).start()

    for j in range(2):

        def body(i, carry, j=j):
            for slot in range(2):
                b = 2 * i + slot
                if j == 0:

                    @pl.when(i > 0)
                    def _():
                        send(j, b, slot, True)

                else:
                    send(j, b, slot, True)
                at = pl.multiple_of(MARGIN + j * shard_rows + b * block, 16)
                out_buf[slot] = stage[pl.ds(at, block), :].astype(jnp.bfloat16)
                send(j, b, slot, False)
            return carry

        repeat(0, 13, body)
    for slot in range(2):
        send(1, 0, slot, True)
    for ref, sem in ((mine, sems.at[0]), (other, sems.at[1])):
        pad = pltpu.make_async_copy(
            zeros, ref.at[pl.ds(shard_rows, padded_rows - shard_rows), :], sem
        )
        pad.start()
        pad.wait()


def half_kernel(core_ref, *refs, low, shard_rows, padded_rows, scale, with_conv):
    high = low + 2 * shard_rows
    matrices, vectors = half_pieces(low, high)
    count = int(with_conv)
    conv_refs, refs = refs[:count], refs[count:]
    mat_refs, refs = refs[: len(matrices)], refs[len(matrices) :]
    vec_refs, refs = refs[: len(vectors)], refs[len(vectors) :]
    mine, other, stage, out_buf, zeros, in_sems, out_sems = refs[:7]
    buffers = {wide: ref for (wide, _), ref in zip(buffer_shapes(matrices), refs[7:])}
    step = pl.program_id(0)

    @pl.when(step == 0)
    def _():
        place_pieces(low, matrices, vectors, mat_refs, vec_refs, stage, buffers, in_sems)
        if low > 0 and not with_conv:
            tail = MARGIN + 2 * shard_rows - 16
            stage[tail : tail + 16, :] = jnp.zeros((16, LANE), jnp.float32)

    if with_conv:
        packed = refs[-1]
        starts, _ = offsets()
        first = MARGIN + starts.pos_weight // LANE - low + step * 2304
        for k in range(3):
            packed[k] = (
                conv_refs[0][:, :, k * LANE : (k + 1) * LANE].reshape(GROUPS * WIDTH, LANE) * scale
            )
        for gh in range(2):
            for cb in range(6):
                outs = swap_slots(
                    [
                        load3(packed, (), pl.ds(gh * 384 + 8 * cb + ci, 8, stride=48))
                        for ci in range(8)
                    ]
                )
                for l in range(8):
                    base = first + l * 288 + gh * 144 + 3 * cb
                    for k in range(3):
                        stage[pl.ds(base + k, 8, stride=18), :] = outs[l][k]

    @pl.when(step == pl.num_programs(0) - 1)
    def _():
        finish_half(
            core_ref[0], shard_rows, padded_rows, stage, mine, other, out_buf, zeros, out_sems
        )


def assemble_half(grads, core, low, shard_rows, padded_rows, with_conv):
    high = low + 2 * shard_rows
    matrices, vectors = half_pieces(low, high)
    args, in_specs = [], []
    if with_conv:
        args.append(Bag(grads).pos_weight)
        in_specs.append(pl.BlockSpec((GROUPS, WIDTH, HALF), lambda i, c: (0, i // 2, i % 2)))
    for key_name, _, _, _, _ in matrices:
        args.append(grads[key_name])
        in_specs.append(pl.BlockSpec(memory_space=pl.ANY))
    for key_name, _, count in vectors:
        args.append(grads[key_name].reshape(1, -1))
        in_specs.append(pl.BlockSpec((1, count * LANE), lambda i, c: (0, 0)))
    block = shard_rows // 26
    scratch = [
        pltpu.VMEM((MARGIN + 2 * shard_rows + 192, LANE), jnp.float32),
        pltpu.VMEM((2, block, LANE), jnp.bfloat16),
        pltpu.VMEM((padded_rows - shard_rows, LANE), jnp.bfloat16),
        pltpu.SemaphoreType.DMA((2,)),
        pltpu.SemaphoreType.DMA((2,)),
    ]
    for wide, rows in buffer_shapes(matrices):
        scratch.append(pltpu.VMEM((2, rows, wide * LANE), jnp.float32))
    if with_conv:
        scratch.append(pltpu.VMEM((3, GROUPS * WIDTH, LANE), jnp.float32))
    out = jax.ShapeDtypeStruct((padded_rows, LANE), jnp.bfloat16)
    return pl.pallas_call(
        functools.partial(
            half_kernel,
            low=low,
            shard_rows=shard_rows,
            padded_rows=padded_rows,
            scale=(TAPS * D // GROUPS) ** (-0.5),
            with_conv=with_conv,
        ),
        grid_spec=pltpu.PrefetchScalarGridSpec(
            num_scalar_prefetch=1,
            grid=(16 if with_conv else 1,),
            in_specs=in_specs,
            out_specs=[pl.BlockSpec(memory_space=pl.ANY)] * 2,
            scratch_shapes=scratch,
        ),
        out_shape=[out, out],
        compiler_params=pltpu.CompilerParams(vmem_limit_bytes=VMEM_MAX),
        cost_estimate=pl.CostEstimate(
            flops=10_000_000, bytes_accessed=40_000_000, transcendentals=0
        ),
    )(core.reshape(1), *args)


CORE_SWAP = [(0, 1), (1, 0), (2, 3), (3, 2)]
Y_SWAP = [(0, 2), (2, 0), (1, 3), (3, 1)]


def pair_half(mine, other):
    arrived = lax.ppermute(other, "shard", CORE_SWAP)
    return (mine.astype(jnp.float32) + arrived.astype(jnp.float32)).astype(jnp.bfloat16)


def reduce_half(pair):
    piece = lax.psum_scatter(pair, "rep", scatter_dimension=0, tiled=True)
    across = lax.ppermute(piece, "shard", Y_SWAP)
    return piece.astype(jnp.float32) + across.astype(jnp.float32)


def padded_shard(shard_rows):
    return -(-shard_rows // 128) * 128


def start_late(grads, shard_rows):
    core = lax.axis_index("shard") % 2
    return pair_half(
        *assemble_half(grads, core, 2 * shard_rows, shard_rows, padded_shard(shard_rows), False)
    )


def combine_chip(grads, late_pair, loss_local, shard_rows):
    spot = lax.axis_index("shard")
    late = reduce_half(late_pair)
    early = reduce_half(
        pair_half(
            *assemble_half(grads, spot % 2, 0, shard_rows, padded_shard(shard_rows), True)
        )
    )
    own = jnp.where(spot < 2, early, late).astype(jnp.bfloat16)
    full = lax.all_gather(own, "rep", axis=0, tiled=True)
    owned = full[:shard_rows].astype(jnp.float32)
    loss = jnp.broadcast_to(loss_local, (8, LANE))
    for step in (1, 2, 4):
        loss = loss + lax.ppermute(loss, "rep", [(i, i ^ step) for i in range(8)])
    sums = jnp.concatenate([jnp.full((8, LANE), jnp.sum(owned * owned)), loss], 0)
    sums = sums + lax.ppermute(sums, "shard", CORE_SWAP)
    sums = sums + lax.ppermute(sums, "shard", Y_SWAP)
    return owned.reshape(-1), sums[0, 0], sums[8, 0]


def combine_any(grads, loss_local, total_params, shard_count, rep_count):
    _, raw_count = offsets()
    shard_rows = total_params // shard_count // LANE
    piece_rows = -(-shard_rows // (rep_count * 16)) * 16
    flat = Bag(grads)
    flat.pos_weight = unpack_weights(
        flat.pos_weight, (TAPS * D // GROUPS) ** (-0.5), jnp.bfloat16
    )
    pieces = [flat[key_name].astype(jnp.bfloat16).reshape(-1, LANE) for key_name, _ in layout()]
    pieces.append(jnp.zeros(((total_params - raw_count) // LANE, LANE), jnp.bfloat16))
    gradient = jnp.concatenate(pieces, 0).reshape(shard_count, shard_rows, LANE)
    gradient = jnp.pad(gradient, ((0, 0), (0, piece_rows * rep_count - shard_rows), (0, 0)))
    reordered = gradient.reshape(shard_count, rep_count, piece_rows, LANE)
    reordered = reordered.transpose(1, 0, 2, 3).reshape(-1, LANE)
    own_piece = lax.psum_scatter(reordered, ("rep", "shard"), scatter_dimension=0, tiled=True)
    own32 = own_piece.astype(jnp.float32)
    square_sum, loss_sum = lax.psum((jnp.sum(own32 * own32), loss_local), ("rep", "shard"))
    owned_grad = lax.all_gather(own_piece, "rep", axis=0, tiled=True)[:shard_rows]
    return owned_grad.reshape(-1).astype(jnp.float32), square_sum, loss_sum


def local(
    frames, segments, padding, masked, distract, targets, params, first_moment, second_moment
):
    shard_count = lax.axis_size("shard")
    rep_count = lax.axis_size("rep")
    full_low = lax.all_gather(params.astype(jnp.bfloat16), "shard", axis=0, tiled=True)
    weights = unpack(full_low)
    starts, raw_count = offsets()
    packed = pack_weights(full_low.reshape(-1, LANE), starts.pos_weight // LANE)
    total_params = full_low.shape[0]
    shard_rows = total_params // shard_count // LANE
    fits = (
        (rep_count, shard_count) == (8, 4)
        and frames.shape[0] == 1
        and shard_rows % 416 == 0
        and 4 * shard_rows - raw_count // LANE == 16
        and (starts.pos_weight + TAPS * D * WIDTH) // LANE <= 2 * shard_rows
    )
    before_conv = (lambda found: start_late(found, shard_rows)) if fits else None
    grads, loss_local, started = None, jnp.float32(0.0), None
    for row in range(frames.shape[0]):
        inputs = [part[row] for part in (frames, segments, padding, masked, distract, targets)]
        grads_row, loss_row, started = row_step(weights, packed, *inputs, before_conv)
        loss_local = loss_local + loss_row
        grads = grads_row if grads is None else jax.tree.map(jnp.add, grads, grads_row)
    if fits:
        owned_grad, square_sum, loss_sum = combine_chip(grads, started, loss_local, shard_rows)
    else:
        owned_grad, square_sum, loss_sum = combine_any(
            grads, loss_local, total_params, shard_count, rep_count
        )
    clip_limit = 12.0 * math.sqrt(
        masked.shape[1] * frames.shape[0] * rep_count * shard_count / FINAL
    )
    grad_norm = jnp.sqrt(square_sum)
    factor = jnp.minimum(1.0, clip_limit / (grad_norm + 1e-06))
    weight_delta, first_new, second_new = adam_update(
        params, owned_grad * factor, first_moment, second_moment
    )
    return (weight_delta, first_new, second_new, grad_norm, loss_sum)


def solution(mesh):
    in_specs = (
        P(("rep", "shard"), None, None),
        P(("rep", "shard"), None),
        P(("rep", "shard"), None),
        P(("rep", "shard"), None),
        P(("rep", "shard"), None, None),
        P(("rep", "shard"), None),
        P("shard"),
        P("shard"),
        P("shard"),
    )
    out_specs = (P("shard"), P("shard"), P("shard"), P(), P())
    return jax.shard_map(local, mesh=mesh, in_specs=in_specs, out_specs=out_specs, check_vma=False)
```

```python
import functools
import math

import jax
import jax.numpy as jnp
from jax import lax
from jax.experimental import pallas as pl
from jax.experimental.pallas import tpu as pltpu
from jax.sharding import PartitionSpec as P

D = 768
HEADS = 12
HEAD_DIM = 64
FF = 3072
FEAT = 512
TAPS = 128
GROUPS = 16
FINAL = 256
CODES = 640
LONG = 750
ROW = 1024


LANE = 128
WIDTH = D // GROUPS
HALF = D // 2
HALF_GROUPS = 8
GAP = TAPS // 2
TQ = ROW + GAP + 16
VMEM_MAX = 66_000_000
UNROLL = 3
highest = lax.Precision.HIGHEST
inverse_temp = 10.0


def layout():
    return [
        ("feat_gain", (FEAT,)),
        ("feat_bias", (FEAT,)),
        ("proj_in", (FEAT, D)),
        ("proj_bias", (D,)),
        ("mask_vector", (D,)),
        ("pos_weight", (TAPS, GROUPS, WIDTH, WIDTH)),
        ("pos_bias", (D,)),
        ("enc_gain", (D,)),
        ("enc_bias", (D,)),
        ("qkv_weight", (D, 3 * D)),
        ("query_bias", (D,)),
        ("value_bias", (D,)),
        ("out_weight", (D, D)),
        ("out_bias", (D,)),
        ("attn_gain", (D,)),
        ("attn_bias", (D,)),
        ("up_weight", (D, FF)),
        ("up_bias", (FF,)),
        ("down_weight", (FF, D)),
        ("down_bias", (D,)),
        ("ffn_gain", (D,)),
        ("ffn_bias", (D,)),
        ("final_weight", (D, FINAL)),
        ("final_bias", (FINAL,)),
        ("codebook", (CODES, FINAL)),
    ]


class Bag(dict):
    __getattr__ = dict.__getitem__
    __setattr__ = dict.__setitem__


def offsets():
    result = Bag()
    offset = 0
    for key_name, dims in layout():
        result[key_name] = offset
        offset += math.prod(dims)
    return result, offset


def unpack(flat):
    starts, _ = offsets()
    result = Bag()
    for key_name, dims in layout():
        if key_name != "pos_weight":
            start = starts[key_name]
            result[key_name] = flat[start : start + math.prod(dims)].reshape(dims)
    return result


def layer_norm(values, gain_raw, bias_raw):
    centered = values - jnp.mean(values, -1, keepdims=True)
    scale_inv = lax.rsqrt(jnp.mean(centered * centered, -1, keepdims=True) + 1e-05)
    return centered * scale_inv * (1.0 + 0.2 * gain_raw) + 0.2 * bias_raw


def gelu_exact(values):
    return jax.nn.gelu(values, approximate=False)


def adam_update(weight_old, grad_scaled, first_old, second_old):
    first_new = 0.5 * first_old + 0.5 * grad_scaled
    second_new = 0.5 * second_old + 0.5 * grad_scaled * grad_scaled
    first_hat = first_new / (1.0 - 0.5**4)
    second_hat = second_new / (1.0 - 0.5**4)
    weight_delta = -0.1 * (first_hat / (jnp.sqrt(second_hat) + 1e-08) + 0.01 * weight_old)
    return (weight_delta, first_new, second_new)


def swap_plan(bit):
    plans = []
    for keep in (0, 1):
        tiles = []
        for v in range(3):
            found = {}
            for lane in range(LANE):
                at = v * LANE + lane
                high = 1 if (at // WIDTH) & bit else 0
                source = at + WIDTH * bit * (keep - high)
                key = (high, source // LANE, (lane - source) % LANE)
                runs = found.setdefault(key, [])
                if runs and runs[-1][1] == lane:
                    runs[-1][1] = lane + 1
                else:
                    runs.append([lane, lane + 1])
            tiles.append(sorted(found.items(), key=lambda e: -sum(h - l for l, h in e[1])))
        plans.append(tiles)
    return plans


PLANS = {bit: swap_plan(bit) for bit in (4, 2, 1)}


def lane_runs(shape, runs):
    lane = lax.broadcasted_iota(jnp.int32, shape, 1)
    result = None
    for low, high in runs:
        part = None
        if low > 0:
            part = lane >= low
        if high < LANE:
            part = lane < high if part is None else part & (lane < high)
        result = part if result is None else result | part
    return result


def swap_half(pair, bit, keep):
    turned = {}

    def source(key):
        array, tile, turn = key
        if key not in turned:
            value = pair[array][tile]
            turned[key] = pltpu.roll(value, turn, 1) if turn else value
        return turned[key]

    result = []
    for entries in PLANS[bit][keep]:
        value = source(entries[0][0])
        for key, runs in entries[1:]:
            value = jnp.where(lane_runs(value.shape, runs), source(key), value)
        result.append(value)
    return result


def swap_slots(arrays):
    arrays = list(arrays)
    for bit in (4, 2, 1):
        done = list(arrays)
        for i in range(8):
            if i & bit == 0:
                pair = (arrays[i], arrays[i | bit])
                done[i] = swap_half(pair, bit, 0)
                done[i | bit] = swap_half(pair, bit, 1)
        arrays = done
    return arrays


def fold_slots(near, far, near_next, far_next, bit):
    kept = swap_half((near, far), bit, 0)
    moved = swap_half((near_next, far_next), bit, 1)
    return [a + b for a, b in zip(kept, moved)]


def repeat(first, last, body):
    count = last - first
    group = next(n for n in (UNROLL, UNROLL - 1, 2, 1) if n > 0 and count % n == 0)

    def several(i, carry):
        for n in range(group):
            body(first + i * group + n, carry)
        return carry

    lax.fori_loop(0, count // group, several, 0)


def load3(ref, lead, rows):
    return [ref[lead + (k, rows)] for k in range(3)]


def store3(ref, lead, rows, value):
    for k in range(3):
        ref[lead + (k, rows)] = value[k]


def weight_pack_kernel(w_ref, o_ref, flat, packed, *, lead):
    flat[...] = w_ref[...].astype(jnp.float32)
    for gh in range(2):
        for cb in range(6):
            taps = []
            for l in range(8):
                base = lead + l * 288 + gh * 144 + 3 * cb
                taps.append([flat[pl.ds(base + k, 8, stride=18), :] for k in range(3)])
            outs = swap_slots(taps)
            for ci in range(8):
                store3(packed, (), pl.ds(gh * 384 + 8 * cb + ci, 8, stride=48), outs[ci])
    for k in range(3):
        o_ref[:, :, k * LANE : (k + 1) * LANE] = (
            packed[k].reshape(GROUPS, WIDTH, LANE).astype(jnp.bfloat16)
        )


def pack_weights(flat_rows, first_row):
    lead = first_row % 16
    start = first_row - lead
    return pl.pallas_call(
        functools.partial(weight_pack_kernel, lead=lead),
        grid=(16,),
        in_specs=[
            pl.BlockSpec((pl.Element(2304 + 16), pl.Element(LANE)), lambda i: (pl.multiple_of(start + 2304 * i, 16), 0))
        ],
        out_specs=pl.BlockSpec((GROUPS, WIDTH, HALF), lambda i: (0, i // 2, i % 2)),
        out_shape=jax.ShapeDtypeStruct((GROUPS, HALF, D), jnp.bfloat16),
        scratch_shapes=[
            pltpu.VMEM((2304 + 16, LANE), jnp.float32),
            pltpu.VMEM((3, GROUPS * WIDTH, LANE), jnp.float32),
        ],
        compiler_params=pltpu.CompilerParams(vmem_limit_bytes=VMEM_MAX),
    )(flat_rows)


def weight_unpack_kernel(w_ref, o_ref, flat, packed, *, scale):
    for k in range(3):
        packed[k] = (
            w_ref[:, :, k * LANE : (k + 1) * LANE].reshape(GROUPS * WIDTH, LANE) * scale
        )
    for gh in range(2):
        for cb in range(6):
            outs = swap_slots(
                [
                    load3(packed, (), pl.ds(gh * 384 + 8 * cb + ci, 8, stride=48))
                    for ci in range(8)
                ]
            )
            for l in range(8):
                base = l * 288 + gh * 144 + 3 * cb
                for k in range(3):
                    flat[pl.ds(base + k, 8, stride=18), :] = outs[l][k]
    o_ref[...] = flat[...].astype(o_ref.dtype)


def unpack_weights(packed, scale, dtype):
    return pl.pallas_call(
        functools.partial(weight_unpack_kernel, scale=scale),
        grid=(16,),
        in_specs=[pl.BlockSpec((GROUPS, WIDTH, HALF), lambda i: (0, i // 2, i % 2))],
        out_specs=pl.BlockSpec((2304, LANE), lambda i: (i, 0)),
        out_shape=jax.ShapeDtypeStruct((16 * 2304, LANE), dtype),
        scratch_shapes=[
            pltpu.VMEM((2304, LANE), jnp.float32),
            pltpu.VMEM((3, GROUPS * WIDTH, LANE), jnp.float32),
        ],
        compiler_params=pltpu.CompilerParams(vmem_limit_bytes=VMEM_MAX),
    )(packed)


def rows_at(start, count):
    return pl.ds(start, count)


def conv_fwd_kernel(edge_ref, x_ref, w_ref, y_ref, xs_ref, xs_all, zs, v_all, c1, d1, e1):
    g = pl.program_id(1)

    @pl.when(g == 0)
    def _():
        def build(i, carry):
            t0 = pl.multiple_of(i * 16, 16)
            outs = swap_slots(
                [
                    [x_ref[pl.ds(t0 + 16 * a, 16), k * LANE : (k + 1) * LANE] for k in range(3)]
                    for a in range(8)
                ]
            )
            for q in range(8):
                for k in range(3):
                    xs_all[q, pl.ds(t0, 16), k * LANE : (k + 1) * LANE] = outs[q][k]
            return carry

        repeat(0, TQ // 16, build)

    xs_ref[0] = xs_all[g]
    for c in range(3):
        z = jnp.dot(
            xs_all[g, c * 368 : (c + 1) * 368, :],
            w_ref[0],
            preferred_element_type=jnp.float32,
        )
        for k in range(6):
            zs[k, c * 368 : (c + 1) * 368, :] = z[:, k * LANE : (k + 1) * LANE]

    def add_high(i, carry):
        t0 = pl.multiple_of(i * 48, 8)
        for k in range(3):
            v_all[g, k, pl.ds(t0, 48), :] = (
                zs[k, pl.ds(t0, 48), :] + zs[k + 3, pl.ds(t0 + 8, 48), :]
            )
        return carry

    repeat(0, TQ // 48, add_high)

    @pl.when(g == HALF_GROUPS - 1)
    def _():
        def fold(src, dst, count, bit):
            def body(i, carry):
                t0 = pl.multiple_of(i * 16, 16)
                for p in range(count):
                    value = fold_slots(
                        load3(src, (p,), pl.ds(t0, 16)),
                        load3(src, (p + count,), pl.ds(t0, 16)),
                        load3(src, (p,), pl.ds(t0 + bit, 16)),
                        load3(src, (p + count,), pl.ds(t0 + bit, 16)),
                        bit,
                    )
                    store3(dst, (p,), pl.ds(t0, 16), value)
                return carry

            return body

        repeat(0, TQ // 16, fold(v_all, c1, 4, 4))
        repeat(0, TQ // 16, fold(c1, d1, 2, 2))
        repeat(0, TQ // 16, fold(d1, e1, 1, 1))
        edge = edge_ref[0]

        def place(i, carry):
            t0 = pl.multiple_of(i * 16, 16)
            row = t0 + lax.broadcasted_iota(jnp.int32, (16, LANE), 0)
            for k in range(3):
                y_ref[pl.ds(t0, 16), k * LANE : (k + 1) * LANE] = jnp.where(
                    row < edge, e1[0, k, pl.ds(t0, 16), :], e1[0, k, pl.ds(t0 + GAP, 16), :]
                )
            return carry

        repeat(0, ROW // 16, place)


def conv_forward(edge, x_gap, packed):
    rows = TQ + 16
    return pl.pallas_call(
        conv_fwd_kernel,
        grid_spec=pltpu.PrefetchScalarGridSpec(
            num_scalar_prefetch=1,
            grid=(2, HALF_GROUPS),
            in_specs=[
                pl.BlockSpec((ROW + 3 * GAP, HALF), lambda h, g, e: (0, h)),
                pl.BlockSpec((1, HALF, D), lambda h, g, e: (h * HALF_GROUPS + g, 0, 0)),
            ],
            out_specs=[
                pl.BlockSpec((ROW, HALF), lambda h, g, e: (0, h)),
                pl.BlockSpec((1, TQ, HALF), lambda h, g, e: (h * HALF_GROUPS + g, 0, 0)),
            ],
            scratch_shapes=[
                pltpu.VMEM((HALF_GROUPS, TQ, HALF), jnp.bfloat16),
                pltpu.VMEM((6, rows, LANE), jnp.float32),
                pltpu.VMEM((8, 3, rows, LANE), jnp.float32),
                pltpu.VMEM((4, 3, rows, LANE), jnp.float32),
                pltpu.VMEM((2, 3, rows, LANE), jnp.float32),
                pltpu.VMEM((1, 3, rows, LANE), jnp.float32),
            ],
        ),
        out_shape=[
            jax.ShapeDtypeStruct((ROW, D), jnp.float32),
            jax.ShapeDtypeStruct((GROUPS, TQ, HALF), jnp.bfloat16),
        ],
        compiler_params=pltpu.CompilerParams(vmem_limit_bytes=VMEM_MAX),
        cost_estimate=pl.CostEstimate(flops=60_000_000_000, bytes_accessed=60_000_000, transcendentals=0),
    )(edge, x_gap, packed)


BACK = ROW + 3 * GAP


def conv_bwd_kernel(
    edge_ref, dy_ref, xs_ref, w_ref, dx_ref, dw_ref, dys, dl, dz, dxs, d1, e1
):
    g = pl.program_id(1)

    @pl.when(g == 0)
    def _():
        def spread(i, carry):
            t0 = pl.multiple_of(i * 16, 16)
            part = dy_ref[pl.ds(t0, 16), :].astype(jnp.float32)
            store3(dys, (), pl.ds(t0, 16), [part[:, k * LANE : (k + 1) * LANE] for k in range(3)])
            return carry

        repeat(0, 1136 // 16, spread)

        def build(i, carry):
            u0 = pl.multiple_of(i * 16, 16)
            outs = swap_slots([load3(dys, (), pl.ds(u0 + 8 - l, 16)) for l in range(8)])
            for q in range(8):
                store3(dl, (q,), pl.ds(u0, 16), outs[q])
            return carry

        repeat(0, 1120 // 16, build)
        zero = jnp.zeros((16, LANE), jnp.float32)

        def clear(i, carry):
            for q in range(8):
                for k in range(3):
                    dxs[q, k, pl.ds(pl.multiple_of(i * 16, 16), 16), :] = zero
            return carry

        repeat(0, GAP // 16, clear)
        repeat((GAP + TQ) // 16, BACK // 16, clear)

    def pack(i, carry):
        t0 = pl.multiple_of(i * 16, 16)
        for k in range(3):
            dz[pl.ds(t0, 16), k * LANE : (k + 1) * LANE] = dl[g, k, pl.ds(t0 + 8, 16), :].astype(
                jnp.bfloat16
            )
            dz[pl.ds(t0, 16), HALF + k * LANE : HALF + (k + 1) * LANE] = dl[
                g, k, pl.ds(t0, 16), :
            ].astype(jnp.bfloat16)
        return carry

    repeat(0, TQ // 16, pack)
    dw_ref[0] = lax.dot_general(
        xs_ref[0], dz[...], (((0,), (0,)), ((), ())), preferred_element_type=jnp.float32
    )
    for c in range(3):
        back = lax.dot_general(
            dz[c * 368 : (c + 1) * 368, :],
            w_ref[0],
            (((1,), (1,)), ((), ())),
            preferred_element_type=jnp.float32,
        )
        for k in range(3):
            dxs[g, k, GAP + c * 368 : GAP + (c + 1) * 368, :] = back[:, k * LANE : (k + 1) * LANE]

    @pl.when(g == HALF_GROUPS - 1)
    def _():
        def fold(src, dst, count, bit, first):
            def body(i, carry):
                t0 = pl.multiple_of(i * 16, 16)
                for p in range(count):
                    value = fold_slots(
                        load3(src, (p,), pl.ds(t0, 16)),
                        load3(src, (p + count,), pl.ds(t0, 16)),
                        load3(src, (p,), pl.ds(t0 - 16 * bit, 16)),
                        load3(src, (p + count,), pl.ds(t0 - 16 * bit, 16)),
                        bit,
                    )
                    store3(dst, (p,), pl.ds(t0, 16), value)
                return carry

            repeat(first // 16, BACK // 16, body)

        fold(dxs, dl, 4, 4, 64)
        fold(dl, d1, 2, 2, 96)
        fold(d1, e1, 1, 1, 112)
        edge = edge_ref[0]

        def place(i, carry):
            t0 = pl.multiple_of(i * 16, 16)
            row = t0 + lax.broadcasted_iota(jnp.int32, (16, LANE), 0)
            for k in range(3):
                dx_ref[pl.ds(t0, 16), k * LANE : (k + 1) * LANE] = jnp.where(
                    row < edge,
                    e1[0, k, pl.ds(t0 + 2 * GAP, 16), :],
                    e1[0, k, pl.ds(t0 + 3 * GAP, 16), :],
                )
            return carry

        repeat(0, ROW // 16, place)


def conv_backward(edge, dy_gap, shifted, packed):
    return pl.pallas_call(
        conv_bwd_kernel,
        grid_spec=pltpu.PrefetchScalarGridSpec(
            num_scalar_prefetch=1,
            grid=(2, HALF_GROUPS),
            in_specs=[
                pl.BlockSpec((1136, HALF), lambda h, g, e: (0, h)),
                pl.BlockSpec((1, TQ, HALF), lambda h, g, e: (h * HALF_GROUPS + g, 0, 0)),
                pl.BlockSpec((1, HALF, D), lambda h, g, e: (h * HALF_GROUPS + g, 0, 0)),
            ],
            out_specs=[
                pl.BlockSpec((ROW, HALF), lambda h, g, e: (0, h)),
                pl.BlockSpec((1, HALF, D), lambda h, g, e: (h * HALF_GROUPS + g, 0, 0)),
            ],
            scratch_shapes=[
                pltpu.VMEM((3, 1136, LANE), jnp.float32),
                pltpu.VMEM((8, 3, BACK, LANE), jnp.float32),
                pltpu.VMEM((TQ, D), jnp.bfloat16),
                pltpu.VMEM((8, 3, BACK, LANE), jnp.float32),
                pltpu.VMEM((2, 3, BACK, LANE), jnp.float32),
                pltpu.VMEM((1, 3, BACK, LANE), jnp.float32),
            ],
        ),
        out_shape=[
            jax.ShapeDtypeStruct((ROW, D), jnp.float32),
            jax.ShapeDtypeStruct((GROUPS, HALF, D), jnp.float32),
        ],
        compiler_params=pltpu.CompilerParams(vmem_limit_bytes=VMEM_MAX),
        cost_estimate=pl.CostEstimate(flops=90_000_000_000, bytes_accessed=80_000_000, transcendentals=0),
    )(edge, dy_gap, shifted, packed)


def with_gap(values, edge, before, total):
    near = jnp.pad(values, ((before, total - ROW - before), (0, 0)))
    far = jnp.pad(values, ((before + GAP, total - ROW - before - GAP), (0, 0)))
    row = lax.broadcasted_iota(jnp.int32, (total, 1), 0) - before
    zero = jnp.zeros((), values.dtype)
    return jnp.where(row < edge, near, jnp.where(row >= edge + GAP, far, zero))


def head_scores(q_ref, k_ref, segq_ref, segk_ref, sub, rows):
    cols = slice(sub * HEAD_DIM, (sub + 1) * HEAD_DIM)
    scores = lax.dot_general(
        q_ref[rows, cols], k_ref[:, cols], (((1,), (1,)), ((), ())),
        preferred_element_type=jnp.float32,
    ) * HEAD_DIM ** (-0.5)
    allowed = segq_ref[rows, :] == segk_ref[...]
    scores = jnp.where(allowed, scores, -1e30)
    power = jnp.exp(scores - jnp.max(scores, -1, keepdims=True))
    return power * (1.0 / jnp.sum(power, -1, keepdims=True))


def attn_fwd_kernel(q_ref, k_ref, v_ref, segq_ref, segk_ref, o_ref):
    for block in range(q_ref.shape[0] // LANE):
        rows = slice(block * LANE, (block + 1) * LANE)
        parts = []
        for sub in range(2):
            probs = head_scores(q_ref, k_ref, segq_ref, segk_ref, sub, rows)
            parts.append(
                jnp.dot(
                    probs.astype(jnp.bfloat16),
                    v_ref[:, sub * HEAD_DIM : (sub + 1) * HEAD_DIM],
                    preferred_element_type=jnp.float32,
                )
            )
        o_ref[rows, :] = jnp.concatenate(parts, 1).astype(jnp.bfloat16)


def attn_bwd_kernel(
    q_ref, k_ref, v_ref, g_ref, segq_ref, segk_ref, dq_ref, dk_ref, dv_ref, probs_low, ds_low
):
    for sub in range(2):
        cols = slice(sub * HEAD_DIM, (sub + 1) * HEAD_DIM)
        for block in range(q_ref.shape[0] // LANE):
            rows = slice(block * LANE, (block + 1) * LANE)
            probs = head_scores(q_ref, k_ref, segq_ref, segk_ref, sub, rows)
            probs_low[rows, :] = probs.astype(jnp.bfloat16)
            grad_probs = lax.dot_general(
                g_ref[rows, cols], v_ref[:, cols], (((1,), (1,)), ((), ())),
                preferred_element_type=jnp.float32,
            )
            total = jnp.sum(probs * grad_probs, -1, keepdims=True)
            ds_low[rows, :] = (probs * (grad_probs - total)).astype(jnp.bfloat16)
        scale = HEAD_DIM ** (-0.5)
        turn = (((0,), (0,)), ((), ()))
        dv_ref[:, cols] = lax.dot_general(
            probs_low[...], g_ref[:, cols], turn, preferred_element_type=jnp.float32
        ).astype(jnp.bfloat16)
        dk_ref[:, cols] = (
            lax.dot_general(
                ds_low[...], q_ref[:, cols], turn, preferred_element_type=jnp.float32
            )
            * scale
        ).astype(jnp.bfloat16)
        dq_ref[:, cols] = (
            jnp.dot(ds_low[...], k_ref[:, cols], preferred_element_type=jnp.float32) * scale
        ).astype(jnp.bfloat16)


def attention(queries, kv, segq, segk):
    count = queries.shape[0]
    pairs = HEADS // 2
    return pl.pallas_call(
        attn_fwd_kernel,
        grid=(pairs,),
        in_specs=[
            pl.BlockSpec((count, LANE), lambda h: (0, h)),
            pl.BlockSpec((ROW, LANE), lambda h: (0, h)),
            pl.BlockSpec((ROW, LANE), lambda h: (0, pairs + h)),
            pl.BlockSpec((count, 1), lambda h: (0, 0)),
            pl.BlockSpec((1, ROW), lambda h: (0, 0)),
        ],
        out_specs=pl.BlockSpec((count, LANE), lambda h: (0, h)),
        out_shape=jax.ShapeDtypeStruct((count, D), jnp.bfloat16),
        compiler_params=pltpu.CompilerParams(vmem_limit_bytes=VMEM_MAX // 2),
    )(queries, kv, kv, segq, segk)


def attention_back(queries, kv, grad, segq, segk):
    count = queries.shape[0]
    pairs = HEADS // 2
    return pl.pallas_call(
        attn_bwd_kernel,
        grid=(pairs,),
        in_specs=[
            pl.BlockSpec((count, LANE), lambda h: (0, h)),
            pl.BlockSpec((ROW, LANE), lambda h: (0, h)),
            pl.BlockSpec((ROW, LANE), lambda h: (0, pairs + h)),
            pl.BlockSpec((count, LANE), lambda h: (0, h)),
            pl.BlockSpec((count, 1), lambda h: (0, 0)),
            pl.BlockSpec((1, ROW), lambda h: (0, 0)),
        ],
        out_specs=[
            pl.BlockSpec((count, LANE), lambda h: (0, h)),
            pl.BlockSpec((ROW, LANE), lambda h: (0, h)),
            pl.BlockSpec((ROW, LANE), lambda h: (0, h)),
        ],
        out_shape=[
            jax.ShapeDtypeStruct((count, D), jnp.bfloat16),
            jax.ShapeDtypeStruct((ROW, D), jnp.bfloat16),
            jax.ShapeDtypeStruct((ROW, D), jnp.bfloat16),
        ],
        scratch_shapes=[
            pltpu.VMEM((count, ROW), jnp.bfloat16),
            pltpu.VMEM((count, ROW), jnp.bfloat16),
        ],
        compiler_params=pltpu.CompilerParams(vmem_limit_bytes=VMEM_MAX // 2),
    )(queries, kv, kv, grad, segq, segk)


def dot_low(left, right):
    return jnp.dot(left, right, preferred_element_type=jnp.float32)


def dot_turn(left, right):
    return lax.dot_general(
        left, right, (((0,), (0,)), ((), ())), preferred_element_type=jnp.float32
    )


def dot_back(left, right):
    return lax.dot_general(
        left, right, (((1,), (1,)), ((), ())), preferred_element_type=jnp.float32
    )


def contrast_counts(masked_row, distract_row, target_row):
    frame = lax.broadcasted_iota(jnp.int32, (1, 1, ROW), 2)
    seen = jnp.sum((distract_row[:, :, None] == frame).astype(jnp.float32), 1)
    code = lax.broadcasted_iota(jnp.int32, (ROW, CODES), 1)
    is_code = (target_row[:, None] == code).astype(jnp.bfloat16)
    counts = dot_low(seen.astype(jnp.bfloat16), is_code)
    pick = (masked_row[:, None] == lax.broadcasted_iota(jnp.int32, (1, ROW), 1)).astype(
        jnp.bfloat16
    )
    own = dot_low(pick, is_code)
    return pick, own, jnp.where(own > 0, 1.0, counts)


def contrast(picked, codebook, own, weight):
    picked_unit = picked * lax.rsqrt(jnp.sum(picked * picked, -1, keepdims=True) + 1e-06)
    code_unit = codebook * lax.rsqrt(jnp.sum(codebook * codebook, -1, keepdims=True) + 1e-06)
    logits = inverse_temp * jnp.dot(
        picked_unit, code_unit.T, precision=highest, preferred_element_type=jnp.float32
    )
    logits = jnp.where(weight > 0, logits, -1e30)
    top = lax.stop_gradient(jnp.max(logits, -1, keepdims=True))
    total = jnp.sum(weight * jnp.exp(logits - top), -1)
    return jnp.sum(top[:, 0] + jnp.log(total) - jnp.sum(own * logits, -1))


def column_sum(rounded):
    return 0.2 * jnp.sum(rounded.astype(jnp.float32), 0)


def row_step(
    weights,
    packed,
    frames_row,
    segment,
    padding_row,
    masked_row,
    distract_row,
    target_row,
    before_conv=None,
):
    vector = Bag((name, part.astype(jnp.float32)) for name, part in weights.items())
    pick, own, weight = contrast_counts(masked_row, distract_row, target_row)
    edge = jnp.sum((segment == 0).astype(jnp.int32)).reshape(1)
    keep_frame = (1 - padding_row).astype(jnp.float32)
    hidden_in, feat_back = jax.vjp(
        layer_norm, frames_row.astype(jnp.float32), vector.feat_gain, vector.feat_bias
    )
    hidden_low = hidden_in.astype(jnp.bfloat16)
    projected = dot_low(hidden_low, weights.proj_in) * FEAT ** (-0.5) + 0.2 * vector.proj_bias
    flagged = jnp.any(
        masked_row[None, :] == lax.broadcasted_iota(jnp.int32, (ROW, 1), 0), 1, keepdims=True
    )
    replaced = jnp.where(flagged, vector.mask_vector[None, :], projected)
    conv_in = (replaced * keep_frame[:, None]).astype(jnp.bfloat16)
    pos_scale = (TAPS * D // GROUPS) ** (-0.5)
    conv_sum, shifted = conv_forward(edge, with_gap(conv_in, edge[0], GAP, ROW + 3 * GAP), packed)
    conv_out = conv_sum * pos_scale + 0.2 * vector.pos_bias
    activated_pos, gelu_pos_back = jax.vjp(gelu_exact, conv_out)
    normed, enc_back = jax.vjp(
        layer_norm, replaced + activated_pos, vector.enc_gain, vector.enc_bias
    )
    normed_low = normed.astype(jnp.bfloat16)
    pick32 = pick.astype(jnp.float32)
    normed_pick = jnp.dot(pick32, normed, precision=highest)
    queries = (
        dot_low(normed_pick.astype(jnp.bfloat16), weights.qkv_weight[:, :D]) * D ** (-0.5)
        + 0.2 * vector.query_bias
    ).astype(jnp.bfloat16)
    kv_bias = jnp.concatenate([jnp.zeros((D,), jnp.float32), 0.2 * vector.value_bias])
    kv_low = (dot_low(normed_low, weights.qkv_weight[:, D:]) * D ** (-0.5) + kv_bias).astype(
        jnp.bfloat16
    )
    segk = jnp.where(padding_row == 0, segment, -1)[None, :]
    segq = jnp.sum(
        pick32 * segment.astype(jnp.float32)[None, :], 1, keepdims=True
    ).astype(jnp.int32)
    mixed_low = attention(queries, kv_low, segq, segk)
    out_scale = (LONG / D) ** 0.5
    attended = dot_low(mixed_low, weights.out_weight) * out_scale + 0.2 * vector.out_bias
    first, attn_back = jax.vjp(
        layer_norm, normed_pick + attended, vector.attn_gain, vector.attn_bias
    )
    first_low = first.astype(jnp.bfloat16)
    hidden_ff = dot_low(first_low, weights.up_weight) * D ** (-0.5) + 0.2 * vector.up_bias
    activated, gelu_ff_back = jax.vjp(gelu_exact, hidden_ff)
    activated_low = activated.astype(jnp.bfloat16)
    branch = dot_low(activated_low, weights.down_weight) * FF ** (-0.5) + 0.2 * vector.down_bias
    second, ffn_back = jax.vjp(layer_norm, first + branch, vector.ffn_gain, vector.ffn_bias)
    second_low = second.astype(jnp.bfloat16)
    context = dot_low(second_low, weights.final_weight) * D ** (-0.5) + 0.2 * vector.final_bias
    loss_row, contrast_back = jax.vjp(
        lambda a, b: contrast(a, b, own, weight), context, vector.codebook
    )
    grad_context, grad_code = contrast_back(jnp.ones_like(loss_row))
    grads = Bag(codebook=grad_code)
    ctx_low = grad_context.astype(jnp.bfloat16)
    grads.final_weight = dot_turn(second_low, ctx_low) * D ** (-0.5)
    grads.final_bias = column_sum(ctx_low)
    grad_second = dot_back(ctx_low, weights.final_weight) * D ** (-0.5)
    grad_res2, grads.ffn_gain, grads.ffn_bias = ffn_back(grad_second)
    branch_low = grad_res2.astype(jnp.bfloat16)
    grads.down_weight = dot_turn(activated_low, branch_low) * FF ** (-0.5)
    grads.down_bias = column_sum(branch_low)
    grad_act = dot_back(branch_low, weights.down_weight) * FF ** (-0.5)
    ff_grad_low = gelu_ff_back(grad_act)[0].astype(jnp.bfloat16)
    grads.up_weight = dot_turn(first_low, ff_grad_low) * D ** (-0.5)
    grads.up_bias = column_sum(ff_grad_low)
    grad_first = grad_res2 + dot_back(ff_grad_low, weights.up_weight) * D ** (-0.5)
    grad_res1, grads.attn_gain, grads.attn_bias = attn_back(grad_first)
    attended_low = grad_res1.astype(jnp.bfloat16)
    grads.out_weight = dot_turn(mixed_low, attended_low) * out_scale
    grads.out_bias = column_sum(attended_low)
    grad_mixed = (dot_back(attended_low, weights.out_weight) * out_scale).astype(jnp.bfloat16)
    grad_q, grad_k, grad_v = attention_back(queries, kv_low, grad_mixed, segq, segk)
    grads.query_bias = column_sum(grad_q)
    grads.value_bias = column_sum(grad_v)
    spread_q = dot_turn(pick, grad_q).astype(jnp.bfloat16)
    qkv_grad_low = jnp.concatenate([spread_q, grad_k, grad_v], 1)
    grads.qkv_weight = dot_turn(normed_low, qkv_grad_low) * D ** (-0.5)
    grad_normed = lax.dot_general(
        pick32, grad_res1, (((0,), (0,)), ((), ())), precision=highest
    ) + dot_back(qkv_grad_low, weights.qkv_weight) * D ** (-0.5)
    grad_embed, grads.enc_gain, grads.enc_bias = enc_back(grad_normed)
    conv_grad_low = gelu_pos_back(grad_embed)[0].astype(jnp.bfloat16)
    grads.pos_bias = column_sum(conv_grad_low)
    grad_gap = with_gap(conv_grad_low, edge[0], 16, 1136)
    started = None
    if before_conv is not None:
        grad_gap, started = lax.optimization_barrier((grad_gap, before_conv(grads)))
    input_grad, packed_grad = conv_backward(edge, grad_gap, shifted, packed)
    grads.pos_weight = packed_grad
    grad_replaced = grad_embed + input_grad * pos_scale * keep_frame[:, None]
    grads.mask_vector = jnp.sum(jnp.where(flagged, grad_replaced, 0.0), 0)
    proj_low = jnp.where(flagged, 0.0, grad_replaced).astype(jnp.bfloat16)
    grads.proj_in = dot_turn(hidden_low, proj_low) * FEAT ** (-0.5)
    grads.proj_bias = column_sum(proj_low)
    grad_hidden = dot_back(proj_low, weights.proj_in) * FEAT ** (-0.5)
    frames_grad, grads.feat_gain, grads.feat_bias = feat_back(grad_hidden)
    return (dict(grads), loss_row, started)


MARGIN = 64
CHUNK = 800 * 1024


def half_pieces(low, high):
    starts, _ = offsets()
    matrices, vectors = [], []
    for key_name, dims in layout():
        if key_name == "pos_weight":
            continue
        first = starts[key_name] // LANE
        count = math.prod(dims) // LANE
        if first >= high or first + count <= low:
            continue
        if len(dims) == 1:
            vectors.append((key_name, first, count))
        else:
            wide = dims[1] // LANE
            begin = max(0, (low - first) // wide // 8 * 8)
            end = min(dims[0], (-(-(high - first) // wide) + 7) // 8 * 8)
            matrices.append((key_name, first, wide, begin, end))
    return matrices, vectors


def chunk_plan(matrices):
    plan = []
    for index, (_, first, wide, begin, end) in enumerate(matrices):
        step = max(8, CHUNK // (wide * LANE * 4) // 8 * 8)
        row = begin
        while row < end:
            count = min(step, end - row)
            plan.append((index, first, wide, row, count))
            row += count
    return plan


def buffer_shapes(matrices):
    return sorted({wide: max(8, CHUNK // (wide * LANE * 4) // 8 * 8) for _, _, wide, _, _ in matrices}.items())


def place_pieces(low, matrices, vectors, refs, vec_refs, stage, buffers, sems):
    plan = chunk_plan(matrices)

    def copy(n):
        index, _, wide, row, count = plan[n]
        slot = n % 2
        return pltpu.make_async_copy(
            refs[index].at[pl.ds(row, count), :],
            buffers[wide].at[slot, pl.ds(0, count), :],
            sems.at[slot],
        )

    copy(0).start()
    for (_, first, count), vec_ref in zip(vectors, vec_refs):
        for k in range(count):
            at = MARGIN + first - low + k
            stage[at : at + 1, :] = vec_ref[:, k * LANE : (k + 1) * LANE]
    for n, (_, first, wide, row, count) in enumerate(plan):
        if n + 1 < len(plan):
            copy(n + 1).start()
        copy(n).wait()
        base = MARGIN + first - low + row * wide
        held = buffers[wide].at[n % 2]

        def body(i, carry, base=base, held=held, wide=wide):
            at = pl.multiple_of(i * 8, 8)
            for k in range(wide):
                stage[pl.ds(base + i * (8 * wide) + k, 8, stride=wide), :] = held[
                    pl.ds(at, 8), k * LANE : (k + 1) * LANE
                ]
            return carry

        repeat(0, count // 8, body)


def finish_half(core, shard_rows, padded_rows, stage, mine, other, out_buf, zeros, sems):
    block = shard_rows // 26
    zeros[...] = jnp.zeros_like(zeros)

    def send(j, b, slot, wait):
        def copy(ref):
            return pltpu.make_async_copy(
                out_buf.at[slot],
                ref.at[pl.ds(pl.multiple_of(b * block, 16), block), :],
                sems.at[slot],
            )

        if wait:
            copy(mine).wait()
        else:

            @pl.when(core == j)
            def _():
                copy(mine).start()

            @pl.when(core != j)
            def _():
                copy(other).start()

    for j in range(2):

        def body(i, carry, j=j):
            for slot in range(2):
                b = 2 * i + slot
                if j == 0:

                    @pl.when(i > 0)
                    def _():
                        send(j, b, slot, True)

                else:
                    send(j, b, slot, True)
                at = pl.multiple_of(MARGIN + j * shard_rows + b * block, 16)
                out_buf[slot] = stage[pl.ds(at, block), :].astype(jnp.bfloat16)
                send(j, b, slot, False)
            return carry

        repeat(0, 13, body)
    for slot in range(2):
        send(1, 0, slot, True)
    for ref, sem in ((mine, sems.at[0]), (other, sems.at[1])):
        pad = pltpu.make_async_copy(
            zeros, ref.at[pl.ds(shard_rows, padded_rows - shard_rows), :], sem
        )
        pad.start()
        pad.wait()


def half_kernel(core_ref, *refs, low, shard_rows, padded_rows, scale, with_conv):
    high = low + 2 * shard_rows
    matrices, vectors = half_pieces(low, high)
    count = int(with_conv)
    conv_refs, refs = refs[:count], refs[count:]
    mat_refs, refs = refs[: len(matrices)], refs[len(matrices) :]
    vec_refs, refs = refs[: len(vectors)], refs[len(vectors) :]
    mine, other, stage, out_buf, zeros, in_sems, out_sems = refs[:7]
    buffers = {wide: ref for (wide, _), ref in zip(buffer_shapes(matrices), refs[7:])}
    step = pl.program_id(0)

    @pl.when(step == 0)
    def _():
        place_pieces(low, matrices, vectors, mat_refs, vec_refs, stage, buffers, in_sems)
        if low > 0 and not with_conv:
            tail = MARGIN + 2 * shard_rows - 16
            stage[tail : tail + 16, :] = jnp.zeros((16, LANE), jnp.float32)

    if with_conv:
        packed = refs[-1]
        starts, _ = offsets()
        first = MARGIN + starts.pos_weight // LANE - low + step * 2304
        for k in range(3):
            packed[k] = (
                conv_refs[0][:, :, k * LANE : (k + 1) * LANE].reshape(GROUPS * WIDTH, LANE) * scale
            )
        for gh in range(2):
            for cb in range(6):
                outs = swap_slots(
                    [
                        load3(packed, (), pl.ds(gh * 384 + 8 * cb + ci, 8, stride=48))
                        for ci in range(8)
                    ]
                )
                for l in range(8):
                    base = first + l * 288 + gh * 144 + 3 * cb
                    for k in range(3):
                        stage[pl.ds(base + k, 8, stride=18), :] = outs[l][k]

    @pl.when(step == pl.num_programs(0) - 1)
    def _():
        finish_half(
            core_ref[0], shard_rows, padded_rows, stage, mine, other, out_buf, zeros, out_sems
        )


def assemble_half(grads, core, low, shard_rows, padded_rows, with_conv):
    high = low + 2 * shard_rows
    matrices, vectors = half_pieces(low, high)
    args, in_specs = [], []
    if with_conv:
        args.append(Bag(grads).pos_weight)
        in_specs.append(pl.BlockSpec((GROUPS, WIDTH, HALF), lambda i, c: (0, i // 2, i % 2)))
    for key_name, _, _, _, _ in matrices:
        args.append(grads[key_name])
        in_specs.append(pl.BlockSpec(memory_space=pl.ANY))
    for key_name, _, count in vectors:
        args.append(grads[key_name].reshape(1, -1))
        in_specs.append(pl.BlockSpec((1, count * LANE), lambda i, c: (0, 0)))
    block = shard_rows // 26
    scratch = [
        pltpu.VMEM((MARGIN + 2 * shard_rows + 192, LANE), jnp.float32),
        pltpu.VMEM((2, block, LANE), jnp.bfloat16),
        pltpu.VMEM((padded_rows - shard_rows, LANE), jnp.bfloat16),
        pltpu.SemaphoreType.DMA((2,)),
        pltpu.SemaphoreType.DMA((2,)),
    ]
    for wide, rows in buffer_shapes(matrices):
        scratch.append(pltpu.VMEM((2, rows, wide * LANE), jnp.float32))
    if with_conv:
        scratch.append(pltpu.VMEM((3, GROUPS * WIDTH, LANE), jnp.float32))
    out = jax.ShapeDtypeStruct((padded_rows, LANE), jnp.bfloat16)
    return pl.pallas_call(
        functools.partial(
            half_kernel,
            low=low,
            shard_rows=shard_rows,
            padded_rows=padded_rows,
            scale=(TAPS * D // GROUPS) ** (-0.5),
            with_conv=with_conv,
        ),
        grid_spec=pltpu.PrefetchScalarGridSpec(
            num_scalar_prefetch=1,
            grid=(16 if with_conv else 1,),
            in_specs=in_specs,
            out_specs=[pl.BlockSpec(memory_space=pl.ANY)] * 2,
            scratch_shapes=scratch,
        ),
        out_shape=[out, out],
        compiler_params=pltpu.CompilerParams(vmem_limit_bytes=VMEM_MAX),
        cost_estimate=pl.CostEstimate(
            flops=10_000_000, bytes_accessed=40_000_000, transcendentals=0
        ),
    )(core.reshape(1), *args)


PARTS = 13


def gather_kernel(own_ref, full_ref, ys, yr, xs, xr, os, ow, cs, cr, ds, dr, keep):
    rep, spot = lax.axis_index("rep"), lax.axis_index("shard")
    rows = own_ref.shape[0]
    half = rows // 2
    part = half // PARTS
    across = (rep, lax.rem(spot + 2, 4))
    beside = (rep + 1 - 2 * lax.rem(rep, 2), spot)
    twin = (rep, spot + 1 - 2 * lax.rem(spot, 2))
    near = lax.rem(rep, 2)
    barrier = pltpu.get_barrier_semaphore()
    for peer in (across, beside, twin):
        pl.semaphore_signal(
            barrier, inc=1, device_id=peer, device_id_type=pl.DeviceIdType.MESH
        )
    pl.semaphore_wait(barrier, 3)

    def send(source, target, send_sem, recv_sem, peer):
        return pltpu.make_async_remote_copy(
            src_ref=source,
            dst_ref=target,
            send_sem=send_sem,
            recv_sem=recv_sem,
            device_id=peer,
            device_id_type=pl.DeviceIdType.MESH,
        )

    def slab(at, count):
        return pl.ds(pl.multiple_of(at, 16), count)

    far = lax.rem(spot + 2, 4) * rows
    direct = []
    for k in range(PARTS):
        at = near * half + k * part
        direct.append(
            send(
                own_ref.at[slab(at, part), :],
                full_ref.at[slab(spot * rows + at, part), :],
                ys.at[k],
                yr.at[k],
                across,
            )
        )
        direct[k].start()
    stay = pltpu.make_async_copy(own_ref, full_ref.at[slab(spot * rows, rows), :], keep)
    stay.start()
    mine = []
    for k in range(2):
        mine.append(
            send(
                own_ref.at[slab(k * half, half), :],
                full_ref.at[slab(spot * rows + k * half, half), :],
                os.at[k],
                ow.at[k],
                twin,
            )
        )
        mine[k].start()
    turned, given, passed = [], [], []

    def pass_on(k):
        turned[k].wait_recv()
        place = full_ref.at[slab(far + (1 - near) * half + k * part, part), :]
        passed.append(send(place, place, ds.at[k], dr.at[k], twin))
        passed[k].start()

    for k in range(PARTS):
        direct[k].wait_recv()
        place = full_ref.at[slab(far + near * half + k * part, part), :]
        turned.append(send(place, place, xs.at[k], xr.at[k], beside))
        turned[k].start()
        given.append(send(place, place, cs.at[k], cr.at[k], twin))
        given[k].start()
        if k > 0:
            pass_on(k - 1)
    pass_on(PARTS - 1)
    stay.wait()
    for copy in mine + given + passed:
        copy.wait_recv()
    for copy in direct + mine + turned + given + passed:
        copy.wait_send()


def gather_params(own):
    rows = own.shape[0]
    sems = pltpu.SemaphoreType.DMA((PARTS,))
    pair = pltpu.SemaphoreType.DMA((2,))
    return pl.pallas_call(
        gather_kernel,
        in_specs=[pl.BlockSpec(memory_space=pltpu.VMEM)],
        out_specs=pl.BlockSpec(memory_space=pl.ANY),
        out_shape=jax.ShapeDtypeStruct((4 * rows, LANE), own.dtype),
        scratch_shapes=[sems, sems, sems, sems, pair, pair, sems, sems, sems, sems]
        + [pltpu.SemaphoreType.DMA],
        compiler_params=pltpu.CompilerParams(collective_id=0, has_side_effects=True),
    )(own)


CORE_SWAP = [(0, 1), (1, 0), (2, 3), (3, 2)]
Y_SWAP = [(0, 2), (2, 0), (1, 3), (3, 1)]


def pair_half(mine, other):
    arrived = lax.ppermute(other, "shard", CORE_SWAP)
    return (mine.astype(jnp.float32) + arrived.astype(jnp.float32)).astype(jnp.bfloat16)


def reduce_half(pair):
    piece = lax.psum_scatter(pair, "rep", scatter_dimension=0, tiled=True)
    across = lax.ppermute(piece, "shard", Y_SWAP)
    return piece.astype(jnp.float32) + across.astype(jnp.float32)


def padded_shard(shard_rows):
    return -(-shard_rows // 128) * 128


def start_late(grads, shard_rows):
    core = lax.axis_index("shard") % 2
    return pair_half(
        *assemble_half(grads, core, 2 * shard_rows, shard_rows, padded_shard(shard_rows), False)
    )


def combine_chip(grads, late_pair, loss_local, shard_rows):
    spot = lax.axis_index("shard")
    late = reduce_half(late_pair)
    early = reduce_half(
        pair_half(
            *assemble_half(grads, spot % 2, 0, shard_rows, padded_shard(shard_rows), True)
        )
    )
    own = jnp.where(spot < 2, early, late).astype(jnp.bfloat16)
    full = lax.all_gather(own, "rep", axis=0, tiled=True)
    owned = full[:shard_rows].astype(jnp.float32)
    loss = jnp.broadcast_to(loss_local, (8, LANE))
    for step in (1, 2, 4):
        loss = loss + lax.ppermute(loss, "rep", [(i, i ^ step) for i in range(8)])
    sums = jnp.concatenate([jnp.full((8, LANE), jnp.sum(owned * owned)), loss], 0)
    sums = sums + lax.ppermute(sums, "shard", CORE_SWAP)
    sums = sums + lax.ppermute(sums, "shard", Y_SWAP)
    return owned.reshape(-1), sums[0, 0], sums[8, 0]


def combine_any(grads, loss_local, total_params, shard_count, rep_count):
    _, raw_count = offsets()
    shard_rows = total_params // shard_count // LANE
    piece_rows = -(-shard_rows // (rep_count * 16)) * 16
    flat = Bag(grads)
    flat.pos_weight = unpack_weights(
        flat.pos_weight, (TAPS * D // GROUPS) ** (-0.5), jnp.bfloat16
    )
    pieces = [flat[key_name].astype(jnp.bfloat16).reshape(-1, LANE) for key_name, _ in layout()]
    pieces.append(jnp.zeros(((total_params - raw_count) // LANE, LANE), jnp.bfloat16))
    gradient = jnp.concatenate(pieces, 0).reshape(shard_count, shard_rows, LANE)
    gradient = jnp.pad(gradient, ((0, 0), (0, piece_rows * rep_count - shard_rows), (0, 0)))
    reordered = gradient.reshape(shard_count, rep_count, piece_rows, LANE)
    reordered = reordered.transpose(1, 0, 2, 3).reshape(-1, LANE)
    own_piece = lax.psum_scatter(reordered, ("rep", "shard"), scatter_dimension=0, tiled=True)
    own32 = own_piece.astype(jnp.float32)
    square_sum, loss_sum = lax.psum((jnp.sum(own32 * own32), loss_local), ("rep", "shard"))
    owned_grad = lax.all_gather(own_piece, "rep", axis=0, tiled=True)[:shard_rows]
    return owned_grad.reshape(-1).astype(jnp.float32), square_sum, loss_sum


def local(
    frames, segments, padding, masked, distract, targets, params, first_moment, second_moment
):
    shard_count = lax.axis_size("shard")
    rep_count = lax.axis_size("rep")
    own_low = params.astype(jnp.bfloat16)
    if (rep_count, shard_count) == (8, 4) and params.shape[0] % (LANE * 416) == 0:
        full_low = gather_params(own_low.reshape(-1, LANE)).reshape(-1)
    else:
        full_low = lax.all_gather(own_low, "shard", axis=0, tiled=True)
    weights = unpack(full_low)
    starts, raw_count = offsets()
    packed = pack_weights(full_low.reshape(-1, LANE), starts.pos_weight // LANE)
    total_params = full_low.shape[0]
    shard_rows = total_params // shard_count // LANE
    fits = (
        (rep_count, shard_count) == (8, 4)
        and frames.shape[0] == 1
        and shard_rows % 416 == 0
        and 4 * shard_rows - raw_count // LANE == 16
        and (starts.pos_weight + TAPS * D * WIDTH) // LANE <= 2 * shard_rows
    )
    before_conv = (lambda found: start_late(found, shard_rows)) if fits else None
    grads, loss_local, started = None, jnp.float32(0.0), None
    for row in range(frames.shape[0]):
        inputs = [part[row] for part in (frames, segments, padding, masked, distract, targets)]
        grads_row, loss_row, started = row_step(weights, packed, *inputs, before_conv)
        loss_local = loss_local + loss_row
        grads = grads_row if grads is None else jax.tree.map(jnp.add, grads, grads_row)
    if fits:
        owned_grad, square_sum, loss_sum = combine_chip(grads, started, loss_local, shard_rows)
    else:
        owned_grad, square_sum, loss_sum = combine_any(
            grads, loss_local, total_params, shard_count, rep_count
        )
    clip_limit = 12.0 * math.sqrt(
        masked.shape[1] * frames.shape[0] * rep_count * shard_count / FINAL
    )
    grad_norm = jnp.sqrt(square_sum)
    factor = jnp.minimum(1.0, clip_limit / (grad_norm + 1e-06))
    weight_delta, first_new, second_new = adam_update(
        params, owned_grad * factor, first_moment, second_moment
    )
    return (weight_delta, first_new, second_new, grad_norm, loss_sum)


def solution(mesh):
    in_specs = (
        P(("rep", "shard"), None, None),
        P(("rep", "shard"), None),
        P(("rep", "shard"), None),
        P(("rep", "shard"), None),
        P(("rep", "shard"), None, None),
        P(("rep", "shard"), None),
        P("shard"),
        P("shard"),
        P("shard"),
    )
    out_specs = (P("shard"), P("shard"), P("shard"), P(), P())
    return jax.shard_map(local, mesh=mesh, in_specs=in_specs, out_specs=out_specs, check_vma=False)
```
